128 devices in a mesh: gx: 16 (over x_lo, z, core), gy: 8 (over y, x_hi).
Axes of the slice: x: 4 (x_hi: 2, x_lo: 2; x = x_hi * 2 + x_lo), y: 4, z: 4, core: 2. Of those that a mesh axis runs over, the one named last changes fastest.
Arguments:
- right_side: float32 [256, 256, 128], P('gx', 'gy'), may hold values from -6 to 6
- shift: float32 [256, 256, 128], P('gx', 'gy'), may hold values from 0.5 to 8
Outputs:
- solution_field: float32 [256, 256, 128], P('gx', 'gy')
- residual: float32 [256, 256, 128], P('gx', 'gy')
The draws below stay inside these ranges and needn't reach their ends.
All inputs are finite; a program needn't handle non-finite values.
Results may differ from the reference program's by a relative error of at most 0.0003.
Values sent between devices are 32-bit elements; how exact they have to be, the bound alone decides.
No kernel may reach another device: no remote copies, remote signals or barrier semaphores. Data moves between devices by JAX's collectives and lax.ppermute only.
A program may use at most 128 MiB of HBM per device.

```python
import math
import jax
import jax.numpy as jnp
from jax import lax

CX = 16
CY = 32
CZ = 128
ITERS = 3
LEVELS = 3
SWEEPS = 2
BOTTOM = 4
NX = 256
NY = 256
N_GX = 16
N_GY = 8


def shard_levels(own_key, dims, cuts, least, top_value):
    def one(dim, blocks):
        steps = jax.random.uniform(jax.random.fold_in(jax.random.fold_in(own_key, 6), dim), (blocks,), jnp.float32, least / len(cuts), top_value / len(cuts))
        return jnp.repeat(jnp.exp(steps), dims[dim] // blocks).reshape((-1,) + (1,) * (len(dims) - dim - 1))

    factor_of = one(*cuts[0])
    for cut in cuts[1:]:
        factor_of = factor_of * one(*cut)
    return factor_of


def normal_values(rng, shape, scale, bound, split=(), held_as=jnp.bfloat16):
    values = scale * jax.random.normal(rng, shape, jnp.float32)
    if split:
        values = values * shard_levels(rng, shape, split, -0.22, 0.18)
    return jnp.clip(values, -bound, bound).astype(held_as)


def setup_inputs(seed: int = 0) -> dict:
    splits = jax.random.split(jax.random.key(seed), 3)
    return {
        "right_side": normal_values(splits[0], (NX, NY, CZ), 1.0, 6.0, ((0, 16), (1, 8)), jnp.float32),
        "shift": jnp.clip(jnp.exp(math.log(8.0) - 2.7725887 * jax.random.uniform(splits[1], (NX, NY, CZ), jnp.float32) ** shard_levels(splits[1], (NX, NY, CZ), ((0, 16), (1, 8)), -0.2, 0.2)), 0.5, 8.0),
    }


relaxation = 0.7
center_weight = 26.0


def neighbours(padded):
    total = padded[:, :, :-2] + padded[:, :, 1:-1] + padded[:, :, 2:]
    total = total[:, :-2] + total[:, 1:-1] + total[:, 2:]
    total = total[:-2] + total[1:-1] + total[2:]
    return total - padded[1:-1, 1:-1, 1:-1]


def coarsen(field):
    first, second, third = field.shape
    return field.reshape(first // 2, 2, second // 2, 2, third // 2, 2).mean(axis=(1, 3, 5))


def prolong(field):
    return jnp.repeat(jnp.repeat(jnp.repeat(field, 2, 0), 2, 1), 2, 2)


def level_diagonals(box_shift):
    result = []
    current = box_shift
    for level in range(LEVELS):
        result.append(center_weight + (4.0 ** level) * current)
        if level + 1 < LEVELS:
            current = coarsen(current)
    return result


def sweep(guess, source, diag):
    return guess + relaxation * (source - (diag * guess - neighbours(jnp.pad(guess, 1)))) / diag


def vcycle(rhs, diags, level):
    diag = diags[level]
    source = (4.0 ** level) * rhs
    count = BOTTOM if level == LEVELS - 1 else SWEEPS
    guess = relaxation * source / diag
    for turn in range(count - 1):
        guess = sweep(guess, source, diag)
    if level < LEVELS - 1:
        leftover = (source - (diag * guess - neighbours(jnp.pad(guess, 1)))) / (4.0 ** level)
        guess = guess + prolong(vcycle(coarsen(leftover), diags, level + 1))
        for turn in range(SWEEPS):
            guess = sweep(guess, source, diag)
    return guess


def precondition(residual, shift):
    widths = ((2, 2), (2, 2), (0, 0))
    res_pad = jnp.pad(residual, widths)
    shift_pad = jnp.pad(shift, widths)
    total = jnp.zeros_like(res_pad)
    extent = (CX + 4, CY + 4, CZ)

    def visit(total, index):
        start_x = ((index // N_GY) * CX).astype(jnp.int32)
        start_y = ((index % N_GY) * CY).astype(jnp.int32)
        start = (start_x, start_y, jnp.zeros((), jnp.int32))
        box = lax.dynamic_slice(res_pad, start, extent)
        box_shift = lax.dynamic_slice(shift_pad, start, extent)
        local = vcycle(box, level_diagonals(box_shift), 0)
        older = lax.dynamic_slice(total, start, extent)
        return lax.dynamic_update_slice(total, older + local, start), None

    total, unused = lax.scan(visit, total, jnp.arange(N_GX * N_GY, dtype=jnp.int32))
    return total[2:-2, 2:-2]


def operate(field, shift):
    return (center_weight + shift) * field - neighbours(jnp.pad(field, 1))


def reference(right_side, shift):
    solution_field = jnp.zeros_like(right_side)
    residual = right_side
    precond = precondition(residual, shift)
    direction = precond
    rz_now = jnp.sum(residual * precond)
    for step in range(ITERS):
        image = operate(direction, shift)
        alpha = rz_now / jnp.sum(direction * image)
        solution_field = solution_field + alpha * direction
        residual = residual - alpha * image
        if step + 1 < ITERS:
            precond = precondition(residual, shift)
            rz_next = jnp.sum(residual * precond)
            direction = precond + (rz_next / rz_now) * direction
            rz_now = rz_next
    return solution_field, residual
```

```python
import jax
import jax.numpy as jnp
from jax import lax
from jax.experimental import pallas as pl
from jax.experimental.pallas import tpu as pltpu
from jax.sharding import PartitionSpec as P

STEP = 0.5
RELAX = 0.7
CENTER = 26.0
AX = ("gx", "gy")
CX, CY, CZ = 16, 32, 128
ROWS = 40
BX = CX + 4
WX = CX + 6
F32 = jnp.float32
YBAND = 5
YROWS = 112
IROWS = 80


def sds(*shape):
    return jax.ShapeDtypeStruct(shape, F32)


def lanes():
    return lax.broadcasted_iota(jnp.int32, (ROWS, CZ), 1)


def rows():
    return lax.broadcasted_iota(jnp.int32, (ROWS, CZ), 0)


def zy_sum(p, sh):
    lane = lanes()
    zs = p + jnp.where(lane >= sh, pltpu.roll(p, sh, 1), 0.0)
    zs = zs + jnp.where(lane < CZ - sh, pltpu.roll(p, CZ - sh, 1), 0.0)
    return zs + pltpu.roll(zs, sh, 0) + pltpu.roll(zs, ROWS - sh, 0)


def stencil(n, sh, load, emit):
    prev = None
    cur = zy_sum(load(0), sh)
    for x in range(n):
        nxt = zy_sum(load(x + 1), sh) if x + 1 < n else None
        total = cur
        if prev is not None:
            total = total + prev
        if nxt is not None:
            total = total + nxt
        emit(x, total)
        prev, cur = cur, nxt


def pair_sum(a, level):
    sh = 2**level
    bit = ((rows() + 7) >> level) & 1
    a = a + jnp.where(bit == 0, pltpu.roll(a, ROWS - sh, 0), pltpu.roll(a, sh, 0))
    bit = (lanes() >> level) & 1
    return a + jnp.where(bit == 0, pltpu.roll(a, CZ - sh, 1), pltpu.roll(a, sh, 1))


def smooth(n, sh, e, g, w):
    def emit(x, total):
        here = e[x]
        e[x] = (1.0 - RELAX) * here + w[x] * (g[x] + (total - here))

    stencil(n, sh, lambda x: e[x], emit)


def restrict(n, level, e, g, dp1, g_next):
    held = []

    def emit(x, total):
        left = (g[x] + total) - dp1[x] * e[x]
        if x % 2 == 0:
            held.append(left)
        else:
            g_next[x // 2] = 0.5 * pair_sum(held.pop() + left, level)

    stencil(n, 2**level, lambda x: e[x], emit)


def vcycle(e0, g0, dp1_0, w0, dp1_1, w1, w2, e1, g1, e2, g2):
    n0, n1, n2 = BX, BX // 2, BX // 4
    for x in range(n0):
        e0[x] = w0[x] * g0[x]
    smooth(n0, 1, e0, g0, w0)
    restrict(n0, 0, e0, g0, dp1_0, g1)
    for x in range(n1):
        e1[x] = w1[x] * g1[x]
    smooth(n1, 2, e1, g1, w1)
    restrict(n1, 1, e1, g1, dp1_1, g2)
    for x in range(n2):
        e2[x] = w2[x] * g2[x]
    for _ in range(3):
        smooth(n2, 4, e2, g2, w2)
    for x in range(n1):
        e1[x] = e1[x] + e2[x // 2]
    for _ in range(2):
        smooth(n1, 2, e1, g1, w1)
    for x in range(n0):
        e0[x] = e0[x] + e1[x // 2]
    for _ in range(2):
        smooth(n0, 1, e0, g0, w0)


def send_x(idx, v, out_a, out_b):
    low, high = 1, CX
    a = jnp.where(idx[0] == 0, high, low)
    b = jnp.where(idx[0] == 0, low, high)
    out_a[...] = v[pl.ds(a, YBAND)]
    out_b[...] = v[pl.ds(b, YBAND)]


def add_x(idx, w, in_a, in_b):
    low, high = 0, CX + 1
    a = jnp.where(idx[0] == 0, high, low)
    b = jnp.where(idx[0] == 0, low, high)
    w[pl.ds(a, YBAND)] = w[pl.ds(a, YBAND)] + in_a[...]
    w[pl.ds(b, YBAND)] = w[pl.ds(b, YBAND)] + in_b[...]


def pack_x_kernel(idx, r, s, out_a, out_b):
    a = jnp.where(idx[0] == 0, CX - 2, 0)
    b = jnp.where(idx[0] == 0, 0, CX - 2)
    out_a[0] = r[pl.ds(a, 2)]
    out_a[1] = s[pl.ds(a, 2)]
    out_b[0] = r[pl.ds(b, 2)]
    out_b[1] = s[pl.ds(b, 2)]


def box_kernel(idx, r, s, in_a, in_b, rbox, sbox, out_a, out_b, pack):
    even = idx[0] == 0
    a = jnp.where(even, CX + 2, 0)
    b = jnp.where(even, 0, CX + 2)
    for k, (src, dst) in enumerate(((r, rbox), (s, sbox))):
        dst[...] = jnp.zeros_like(dst)
        for x in range(CX):
            dst[x + 2, 3 : 3 + CY, :] = src[x]
        for x in range(2):
            dst[a + x, 3 : 3 + CY, :] = in_a[k, x]
            dst[b + x, 3 : 3 + CY, :] = in_b[k, x]
        for x in range(BX):
            pack[0, 4 * x + 2 * k : 4 * x + 2 * k + 2, :] = dst[x, 3:5, :]
            pack[1, 4 * x + 2 * k : 4 * x + 2 * k + 2, :] = dst[x, 33:35, :]
    up = jnp.where(idx[1] == 0, 1, 0)
    out_a[...] = pack[up]
    out_b[...] = pack[1 - up]


def first_kernel(
    idx, rin, sin, in_a, in_b,
    r0, v, out_a, out_b, dp1_0, w0, dp1_1, w1, w2,
    got, s0, s1, e1, g1, e2, g2,
):
    up = jnp.where(idx[1] == 0, 1, 0)
    got[up] = in_a[...]
    got[1 - up] = in_b[...]
    row = rows()
    inside = (row >= 1) & (row < 37)
    for k, (src, dst) in enumerate(((rin, r0), (sin, s0))):
        dst[...] = src[...]
        for x in range(BX):
            dst[x, 1:3, :] = got[0, 4 * x + 2 * k : 4 * x + 2 * k + 2, :]
            dst[x, 35:37, :] = got[1, 4 * x + 2 * k : 4 * x + 2 * k + 2, :]

    def coefficients(n, scale, s, dp1, w):
        for x in range(n):
            d = CENTER + scale * s[x]
            if dp1 is not None:
                dp1[x] = d + 1.0
            w[x] = jnp.where(inside, RELAX / d, 0.0)

    coefficients(BX, 1.0, s0, dp1_0, w0)
    for x in range(BX // 2):
        s1[x] = 0.125 * pair_sum(s0[2 * x] + s0[2 * x + 1], 0)
    coefficients(BX // 2, 4.0, s1, dp1_1, w1)
    for x in range(BX // 4):
        s0[x] = 0.125 * pair_sum(s1[2 * x] + s1[2 * x + 1], 1)
    coefficients(BX // 4, 16.0, s0, None, w2)
    v[0] = jnp.zeros((ROWS, CZ), F32)
    v[WX - 1] = jnp.zeros((ROWS, CZ), F32)
    vcycle(v.at[pl.ds(1, BX)], r0, dp1_0, w0, dp1_1, w1, w2, e1, g1, e2, g2)
    send_x(idx, v, out_a, out_b)


def pack_y_kernel(idx, v, in_a, in_b, out_a, out_b, w, pack):
    for x in range(WX):
        w[x, 0:8, :] = v[x, 0:8, :]
        w[x, 8:16, :] = v[x, 32:40, :]
    a = jnp.where(idx[0] == 0, CX + 1, 0)
    b = jnp.where(idx[0] == 0, 0, CX + 1)
    for first, src in ((a, in_a), (b, in_b)):
        for x in range(YBAND):
            w[first + x, 0:8, :] = w[first + x, 0:8, :] + src[x, 0:8, :]
            w[first + x, 8:16, :] = w[first + x, 8:16, :] + src[x, 32:40, :]
    pack[:, YROWS - 8 :, :] = jnp.zeros((2, 8, CZ), F32)
    for x in range(WX):
        pack[0, YBAND * x : YBAND * x + YBAND, :] = w[x, 1:6, :]
        pack[1, YBAND * x : YBAND * x + YBAND, :] = w[x, 8:13, :]
    up = jnp.where(idx[1] == 0, 1, 0)
    out_a[...] = pack[up]
    out_b[...] = pack[1 - up]


def assemble(idx, w, v, xa, xb, ya, yb, got):
    w[...] = v[...]
    add_x(idx, w, xa, xb)
    up = jnp.where(idx[1] == 0, 1, 0)
    got[up] = ya[...]
    got[1 - up] = yb[...]
    row = rows()
    mask = jnp.where(((row >= 3) | (idx[4] == 0)) & ((row < 3 + CY) | (idx[5] == 0)), 1.0, 0.0)
    for x in range(WX):
        w[x, 0:5, :] = w[x, 0:5, :] + got[0, YBAND * x : YBAND * x + YBAND, :]
        w[x, 33:38, :] = w[x, 33:38, :] + got[1, YBAND * x : YBAND * x + YBAND, :]
        m = mask
        if x < 3:
            m = mask * jnp.where(idx[2] == 0, 1.0, 0.0)
        if x >= CX + 3:
            m = mask * jnp.where(idx[3] == 0, 1.0, 0.0)
        w[x] = w[x] * m


def box_mask(idx, x):
    row = rows()
    low = jnp.where(idx[4] == 0, 1, 3)
    high = jnp.where(idx[5] == 0, 37, 35)
    m = jnp.where((row >= low) & (row < high), 1.0, 0.0)
    if x < 2:
        m = m * jnp.where(idx[2] == 0, 1.0, 0.0)
    if x >= CX + 2:
        m = m * jnp.where(idx[3] == 0, 1.0, 0.0)
    return m


def next_kernel(
    idx, vin, xa, xb, ya, yb, rin, dp1_0, w0, dp1_1, w1, w2,
    z, r, v, out_a, out_b,
    w, got, e1, g1, e2, g2,
):
    assemble(idx, w, vin, xa, xb, ya, yb, got)
    z[...] = w[pl.ds(3, CX)]

    def emit(x, total):
        if 1 <= x <= BX:
            image = dp1_0[x - 1] * w[x] - total
            r[x - 1] = rin[x - 1] - (STEP * box_mask(idx, x - 1)) * image

    stencil(WX, 1, lambda x: w[x], emit)
    v[0] = jnp.zeros((ROWS, CZ), F32)
    v[WX - 1] = jnp.zeros((ROWS, CZ), F32)
    vcycle(v.at[pl.ds(1, BX)], r, dp1_0, w0, dp1_1, w1, w2, e1, g1, e2, g2)
    send_x(idx, v, out_a, out_b)


def dots_kernel(idx, vin, xa, xb, ya, yb, dp1_0, z0, z1, r0, r1, r2, z2, u2, sums, w, got):
    assemble(idx, w, vin, xa, xb, ya, yb, got)

    def emit(x, total):
        if 3 <= x < 3 + CX:
            z2[x - 3] = w[x]
            u2[x - 3] = dp1_0[x - 1] * w[x] - total

    stencil(WX, 1, lambda x: w[x], emit)
    row = rows()
    own = jnp.where((row >= 3) & (row < 3 + CY), 1.0, 0.0)
    acc = [jnp.zeros((ROWS, CZ), F32) for _ in range(7)]
    for x in range(CX):
        a0, a1, a2 = z0[x] * own, z1[x] * own, z2[x] * own
        b0, b1, b2 = r0[x + 2], r1[x + 2], r2[x + 2]
        terms = (a0 * b0, a0 * b1, a0 * b2, a1 * b1, a1 * b2, a2 * b2, a2 * u2[x])
        acc = [s + t for s, t in zip(acc, terms)]
    lane = lax.broadcasted_iota(jnp.int32, (1, CZ), 1)
    out = jnp.zeros((1, CZ), F32)
    for k, s in enumerate(acc):
        part = jnp.sum(jnp.sum(s, axis=0, keepdims=True), axis=1, keepdims=True)
        out = out + jnp.where(lane == k, part, 0.0)
    sums[...] = jnp.broadcast_to(out, sums.shape)


def final_kernel(gathered, z0, z1, z2, r0, r1, r2, u2, x_out, r_out):
    row = jnp.sum(gathered[...], axis=0, keepdims=True)
    lane = lax.broadcasted_iota(jnp.int32, (1, CZ), 1)
    m00, m01, m02, m11, m12, m22, h22 = (
        jnp.sum(jnp.where(lane == k, row, 0.0), axis=1, keepdims=True) for k in range(7)
    )
    inv = 1.0 / STEP
    h00, h01, h02 = inv * (m00 - m01), inv * (m01 - m02), inv * (m02 - m12)
    h11, h12 = inv * (m11 - m12), inv * (m12 - m22)
    l10, l20 = h01 / h00, h02 / h00
    d1 = h11 - l10 * h01
    q = h12 - l10 * h02
    l21 = q / d1
    d2 = h22 - l20 * h02 - l21 * q
    y1 = m01 - l10 * m00
    y2 = m02 - l20 * m00 - l21 * y1
    c2 = y2 / d2
    c1 = y1 / d1 - l21 * c2
    c0 = m00 / h00 - l10 * c1 - l20 * c2
    f0, f1 = inv * c0, inv * c1
    for x in range(CX):
        xs = c0 * z0[x] + c1 * z1[x] + c2 * z2[x]
        b0, b1 = r0[x + 2], r1[x + 2]
        rs = b0 - f0 * (b0 - b1) - f1 * (b1 - r2[x + 2]) - c2 * u2[x]
        x_out[x] = xs[3 : 3 + CY, :]
        r_out[x] = rs[3 : 3 + CY, :]


def vmem(n):
    return [pl.BlockSpec(memory_space=pltpu.VMEM) for _ in range(n)]


def call(body, name, n_in, outs, scratch=(), smem=True):
    in_specs = ([pl.BlockSpec(memory_space=pltpu.SMEM)] if smem else []) + vmem(n_in)
    return pl.pallas_call(
        body,
        out_shape=outs,
        in_specs=in_specs,
        out_specs=vmem(len(outs)),
        scratch_shapes=[pltpu.VMEM(s, F32) for s in scratch],
        name=name,
        interpret=INTERPRET,
    )


INTERPRET = False


def pairs(n_gx, n_gy, axis, odd):
    count = n_gx if axis == 0 else n_gy
    result = []
    for i in range(n_gx):
        for j in range(n_gy):
            here = i if axis == 0 else j
            there = ((here + odd) ^ 1) - odd
            if 0 <= there < count:
                target = (there, j) if axis == 0 else (i, there)
                result.append((i * n_gy + j, target[0] * n_gy + target[1]))
    return result


def solution(mesh):
    n_gx, n_gy = mesh.shape["gx"], mesh.shape["gy"]

    def swap(a, b, axis):
        return (
            lax.ppermute(a, AX, pairs(n_gx, n_gy, axis, 0)),
            lax.ppermute(b, AX, pairs(n_gx, n_gy, axis, 1)),
        )

    box = sds(BX, ROWS, CZ)
    half = sds(BX // 2, ROWS, CZ)
    quarter = sds(BX // 4, ROWS, CZ)
    wide = sds(WX, ROWS, CZ)
    band = sds(YBAND, ROWS, CZ)
    yband = sds(YROWS, CZ)
    own = sds(CX, ROWS, CZ)
    coarse = [half.shape, half.shape, quarter.shape, quarter.shape]

    def on_device(right_side, shift):
        gx, gy = lax.axis_index("gx"), lax.axis_index("gy")
        idx = jnp.stack(
            [gx % 2, gy % 2]
            + [(c).astype(jnp.int32) for c in (gx == 0, gx == n_gx - 1, gy == 0, gy == n_gy - 1)]
        )

        def exchange_y(v, xa, xb):
            return swap(
                *call(
                    pack_y_kernel, "pack_y", 3, [yband, yband], [(WX, 16, CZ), (2, YROWS, CZ)]
                )(idx, v, xa, xb),
                1,
            )

        first = sds(2, 2, CY, CZ)
        xa, xb = swap(*call(pack_x_kernel, "pack_x", 2, [first, first])(idx, right_side, shift), 0)
        strip = sds(IROWS, CZ)
        rbox, sbox, ya, yb = call(
            box_kernel, "box", 4, [box, box, strip, strip], [(2, IROWS, CZ)]
        )(idx, right_side, shift, xa, xb)
        ya, yb = swap(ya, yb, 1)
        r0, v, xa, xb, *coefs = call(
            first_kernel,
            "first",
            4,
            [box, wide, band, band, box, box, half, half, quarter],
            [(2, IROWS, CZ), box.shape, half.shape] + coarse,
        )(idx, rbox, sbox, ya, yb)
        residuals, images = [r0], []
        for step in range(2):
            xa, xb = swap(xa, xb, 0)
            ya, yb = exchange_y(v, xa, xb)
            z, r, v, xa, xb = call(
                next_kernel,
                "next",
                11,
                [own, box, wide, band, band],
                [wide.shape, (2, YROWS, CZ)] + coarse,
            )(idx, v, xa, xb, ya, yb, residuals[-1], *coefs)
            images.append(z)
            residuals.append(r)
        xa, xb = swap(xa, xb, 0)
        ya, yb = exchange_y(v, xa, xb)
        z2, u2, sums = call(
            dots_kernel,
            "dots",
            11,
            [own, own, sds(n_gx * n_gy, CZ)],
            [wide.shape, (2, YROWS, CZ)],
        )(idx, v, xa, xb, ya, yb, coefs[0], *images, *residuals)
        gathered = lax.all_to_all(sums, AX, 0, 0, tiled=True)
        x, r = call(
            final_kernel, "final", 8, [sds(CX, CY, CZ), sds(CX, CY, CZ)], smem=False
        )(gathered, *images, z2, *residuals, u2)
        return x, r

    spec = P("gx", "gy", None)
    return jax.shard_map(
        on_device, mesh=mesh, in_specs=(spec, spec), out_specs=(spec, spec), check_vma=False
    )
```

```python
import jax
import jax.numpy as jnp
from jax import lax
from jax.experimental import pallas as pl
from jax.experimental.pallas import tpu as pltpu
from jax.sharding import PartitionSpec as P

STEP = 0.5
RELAX = 0.7
CENTER = 26.0
AX = ("gx", "gy")
CX, CY, CZ = 16, 32, 128
ROWS = 40
BX = CX + 4
WX = CX + 6
F32 = jnp.float32
YBAND = 5
YROWS = 112
IROWS = 80


def sds(*shape):
    return jax.ShapeDtypeStruct(shape, F32)


def lanes():
    return lax.broadcasted_iota(jnp.int32, (ROWS, CZ), 1)


def rows():
    return lax.broadcasted_iota(jnp.int32, (ROWS, CZ), 0)


def zy_sum(p, sh):
    lane = lanes()
    zs = p + jnp.where(lane >= sh, pltpu.roll(p, sh, 1), 0.0)
    zs = zs + jnp.where(lane < CZ - sh, pltpu.roll(p, CZ - sh, 1), 0.0)
    return zs + pltpu.roll(zs, sh, 0) + pltpu.roll(zs, ROWS - sh, 0)


def stencil(n, sh, load, emit):
    prev = None
    cur = zy_sum(load(0), sh)
    for x in range(n):
        nxt = zy_sum(load(x + 1), sh) if x + 1 < n else None
        total = cur
        if prev is not None:
            total = total + prev
        if nxt is not None:
            total = total + nxt
        emit(x, total)
        prev, cur = cur, nxt


def pair_sum(a, level):
    sh = 2**level
    bit = ((rows() + 7) >> level) & 1
    a = a + jnp.where(bit == 0, pltpu.roll(a, ROWS - sh, 0), pltpu.roll(a, sh, 0))
    bit = (lanes() >> level) & 1
    return a + jnp.where(bit == 0, pltpu.roll(a, CZ - sh, 1), pltpu.roll(a, sh, 1))


def smooth(n, sh, e, g, w):
    def emit(x, total):
        here = e[x]
        e[x] = (1.0 - RELAX) * here + w[x] * (g[x] + (total - here))

    stencil(n, sh, lambda x: e[x], emit)


def restrict(n, level, e, g, dp1, g_next):
    held = []

    def emit(x, total):
        left = (g[x] + total) - dp1[x] * e[x]
        if x % 2 == 0:
            held.append(left)
        else:
            g_next[x // 2] = 0.5 * pair_sum(held.pop() + left, level)

    stencil(n, 2**level, lambda x: e[x], emit)


def vcycle(e0, g0, dp1_0, w0, dp1_1, w1, w2, e1, g1, e2, g2):
    n0, n1, n2 = BX, BX // 2, BX // 4
    for x in range(n0):
        e0[x] = w0[x] * g0[x]
    smooth(n0, 1, e0, g0, w0)
    restrict(n0, 0, e0, g0, dp1_0, g1)
    for x in range(n1):
        e1[x] = w1[x] * g1[x]
    smooth(n1, 2, e1, g1, w1)
    restrict(n1, 1, e1, g1, dp1_1, g2)
    for x in range(n2):
        e2[x] = w2[x] * g2[x]
    for _ in range(3):
        smooth(n2, 4, e2, g2, w2)
    for x in range(n1):
        e1[x] = e1[x] + e2[x // 2]
    for _ in range(2):
        smooth(n1, 2, e1, g1, w1)
    for x in range(n0):
        e0[x] = e0[x] + e1[x // 2]
    for _ in range(2):
        smooth(n0, 1, e0, g0, w0)


def send_x(idx, v, out_a, out_b):
    low, high = 1, CX
    a = jnp.where(idx[0] == 0, high, low)
    b = jnp.where(idx[0] == 0, low, high)
    out_a[...] = v[pl.ds(a, YBAND)]
    out_b[...] = v[pl.ds(b, YBAND)]


def add_x(idx, w, in_a, in_b):
    low, high = 0, CX + 1
    a = jnp.where(idx[0] == 0, high, low)
    b = jnp.where(idx[0] == 0, low, high)
    w[pl.ds(a, YBAND)] = w[pl.ds(a, YBAND)] + in_a[...]
    w[pl.ds(b, YBAND)] = w[pl.ds(b, YBAND)] + in_b[...]


def pack_x_kernel(idx, r, s, out_a, out_b):
    a = jnp.where(idx[0] == 0, CX - 2, 0)
    b = jnp.where(idx[0] == 0, 0, CX - 2)
    out_a[0] = r[pl.ds(a, 2)]
    out_a[1] = s[pl.ds(a, 2)]
    out_b[0] = r[pl.ds(b, 2)]
    out_b[1] = s[pl.ds(b, 2)]


def box_kernel(idx, r, s, in_a, in_b, rbox, sbox, out_a, out_b, pack):
    even = idx[0] == 0
    a = jnp.where(even, CX + 2, 0)
    b = jnp.where(even, 0, CX + 2)
    for k, (src, dst) in enumerate(((r, rbox), (s, sbox))):
        dst[...] = jnp.zeros_like(dst)
        for x in range(CX):
            dst[x + 2, 3 : 3 + CY, :] = src[x]
        for x in range(2):
            dst[a + x, 3 : 3 + CY, :] = in_a[k, x]
            dst[b + x, 3 : 3 + CY, :] = in_b[k, x]
        for x in range(BX):
            pack[0, 4 * x + 2 * k : 4 * x + 2 * k + 2, :] = dst[x, 3:5, :]
            pack[1, 4 * x + 2 * k : 4 * x + 2 * k + 2, :] = dst[x, 33:35, :]
    up = jnp.where(idx[1] == 0, 1, 0)
    out_a[...] = pack[up]
    out_b[...] = pack[1 - up]


def first_kernel(
    idx, rin, sin, in_a, in_b,
    r0, v, out_a, out_b, dp1_0, w0, dp1_1, w1, w2,
    got, s0, s1, e1, g1, e2, g2,
):
    up = jnp.where(idx[1] == 0, 1, 0)
    got[up] = in_a[...]
    got[1 - up] = in_b[...]
    row = rows()
    inside = (row >= 1) & (row < 37)
    for k, (src, dst) in enumerate(((rin, r0), (sin, s0))):
        dst[...] = src[...]
        for x in range(BX):
            dst[x, 1:3, :] = got[0, 4 * x + 2 * k : 4 * x + 2 * k + 2, :]
            dst[x, 35:37, :] = got[1, 4 * x + 2 * k : 4 * x + 2 * k + 2, :]

    def coefficients(n, scale, s, dp1, w):
        for x in range(n):
            d = CENTER + scale * s[x]
            if dp1 is not None:
                dp1[x] = d + 1.0
            w[x] = jnp.where(inside, RELAX / d, 0.0)

    coefficients(BX, 1.0, s0, dp1_0, w0)
    for x in range(BX // 2):
        s1[x] = 0.125 * pair_sum(s0[2 * x] + s0[2 * x + 1], 0)
    coefficients(BX // 2, 4.0, s1, dp1_1, w1)
    for x in range(BX // 4):
        s0[x] = 0.125 * pair_sum(s1[2 * x] + s1[2 * x + 1], 1)
    coefficients(BX // 4, 16.0, s0, None, w2)
    v[0] = jnp.zeros((ROWS, CZ), F32)
    v[WX - 1] = jnp.zeros((ROWS, CZ), F32)
    vcycle(v.at[pl.ds(1, BX)], r0, dp1_0, w0, dp1_1, w1, w2, e1, g1, e2, g2)
    send_x(idx, v, out_a, out_b)


def pack_y_kernel(idx, v, in_a, in_b, out_a, out_b, w, pack):
    for x in range(WX):
        w[x, 0:8, :] = v[x, 0:8, :]
        w[x, 8:16, :] = v[x, 32:40, :]
    a = jnp.where(idx[0] == 0, CX + 1, 0)
    b = jnp.where(idx[0] == 0, 0, CX + 1)
    for first, src in ((a, in_a), (b, in_b)):
        for x in range(YBAND):
            w[first + x, 0:8, :] = w[first + x, 0:8, :] + src[x, 0:8, :]
            w[first + x, 8:16, :] = w[first + x, 8:16, :] + src[x, 32:40, :]
    pack[:, YROWS - 8 :, :] = jnp.zeros((2, 8, CZ), F32)
    for x in range(WX):
        pack[0, YBAND * x : YBAND * x + YBAND, :] = w[x, 1:6, :]
        pack[1, YBAND * x : YBAND * x + YBAND, :] = w[x, 8:13, :]
    up = jnp.where(idx[1] == 0, 1, 0)
    out_a[...] = pack[up]
    out_b[...] = pack[1 - up]


def assemble(idx, w, v, xa, xb, ya, yb, got):
    w[...] = v[...]
    add_x(idx, w, xa, xb)
    up = jnp.where(idx[1] == 0, 1, 0)
    got[up] = ya[...]
    got[1 - up] = yb[...]
    row = rows()
    mask = jnp.where(((row >= 3) | (idx[4] == 0)) & ((row < 3 + CY) | (idx[5] == 0)), 1.0, 0.0)
    for x in range(WX):
        w[x, 0:5, :] = w[x, 0:5, :] + got[0, YBAND * x : YBAND * x + YBAND, :]
        w[x, 33:38, :] = w[x, 33:38, :] + got[1, YBAND * x : YBAND * x + YBAND, :]
        m = mask
        if x < 3:
            m = mask * jnp.where(idx[2] == 0, 1.0, 0.0)
        if x >= CX + 3:
            m = mask * jnp.where(idx[3] == 0, 1.0, 0.0)
        w[x] = w[x] * m


def box_mask(idx, x):
    row = rows()
    low = jnp.where(idx[4] == 0, 1, 3)
    high = jnp.where(idx[5] == 0, 37, 35)
    m = jnp.where((row >= low) & (row < high), 1.0, 0.0)
    if x < 2:
        m = m * jnp.where(idx[2] == 0, 1.0, 0.0)
    if x >= CX + 2:
        m = m * jnp.where(idx[3] == 0, 1.0, 0.0)
    return m


def next_kernel(
    idx, vin, xa, xb, ya, yb, rin, dp1_0, w0, dp1_1, w1, w2,
    z, r, v, out_a, out_b,
    w, got, e1, g1, e2, g2,
):
    assemble(idx, w, vin, xa, xb, ya, yb, got)
    z[...] = w[pl.ds(3, CX)]

    def emit(x, total):
        if 1 <= x <= BX:
            image = dp1_0[x - 1] * w[x] - total
            r[x - 1] = rin[x - 1] - (STEP * box_mask(idx, x - 1)) * image

    stencil(WX, 1, lambda x: w[x], emit)
    v[0] = jnp.zeros((ROWS, CZ), F32)
    v[WX - 1] = jnp.zeros((ROWS, CZ), F32)
    vcycle(v.at[pl.ds(1, BX)], r, dp1_0, w0, dp1_1, w1, w2, e1, g1, e2, g2)
    send_x(idx, v, out_a, out_b)


def dots_kernel(idx, vin, xa, xb, ya, yb, dp1_0, z0, z1, r0, r1, r2, z2, u2, sums, w, got):
    assemble(idx, w, vin, xa, xb, ya, yb, got)

    def emit(x, total):
        if 3 <= x < 3 + CX:
            z2[x - 3] = w[x]
            u2[x - 3] = dp1_0[x - 1] * w[x] - total

    stencil(WX, 1, lambda x: w[x], emit)
    row = rows()
    own = jnp.where((row >= 3) & (row < 3 + CY), 1.0, 0.0)
    acc = [jnp.zeros((ROWS, CZ), F32) for _ in range(7)]
    for x in range(CX):
        a0, a1, a2 = z0[x] * own, z1[x] * own, z2[x] * own
        b0, b1, b2 = r0[x + 2], r1[x + 2], r2[x + 2]
        terms = (a0 * b0, a0 * b1, a0 * b2, a1 * b1, a1 * b2, a2 * b2, a2 * u2[x])
        acc = [s + t for s, t in zip(acc, terms)]
    lane = lax.broadcasted_iota(jnp.int32, (1, CZ), 1)
    out = jnp.zeros((1, CZ), F32)
    for k, s in enumerate(acc):
        part = jnp.sum(jnp.sum(s, axis=0, keepdims=True), axis=1, keepdims=True)
        out = out + jnp.where(lane == k, part, 0.0)
    sums[...] = jnp.broadcast_to(out, sums.shape)


def final_kernel(gathered, z0, z1, z2, r0, r1, r2, u2, x_out, r_out):
    row = jnp.sum(gathered[...], axis=0, keepdims=True)
    lane = lax.broadcasted_iota(jnp.int32, (1, CZ), 1)
    m00, m01, m02, m11, m12, m22, h22 = (
        jnp.sum(jnp.where(lane == k, row, 0.0), axis=1, keepdims=True) for k in range(7)
    )
    inv = 1.0 / STEP
    h00, h01, h02 = inv * (m00 - m01), inv * (m01 - m02), inv * (m02 - m12)
    h11, h12 = inv * (m11 - m12), inv * (m12 - m22)
    l10, l20 = h01 / h00, h02 / h00
    d1 = h11 - l10 * h01
    q = h12 - l10 * h02
    l21 = q / d1
    d2 = h22 - l20 * h02 - l21 * q
    y1 = m01 - l10 * m00
    y2 = m02 - l20 * m00 - l21 * y1
    c2 = y2 / d2
    c1 = y1 / d1 - l21 * c2
    c0 = m00 / h00 - l10 * c1 - l20 * c2
    f0, f1 = inv * c0, inv * c1
    for x in range(CX):
        xs = c0 * z0[x] + c1 * z1[x] + c2 * z2[x]
        b0, b1 = r0[x + 2], r1[x + 2]
        rs = b0 - f0 * (b0 - b1) - f1 * (b1 - r2[x + 2]) - c2 * u2[x]
        x_out[x] = xs[3 : 3 + CY, :]
        r_out[x] = rs[3 : 3 + CY, :]


def vmem(n):
    return [pl.BlockSpec(memory_space=pltpu.VMEM) for _ in range(n)]


def call(body, name, n_in, outs, scratch=(), smem=True):
    in_specs = ([pl.BlockSpec(memory_space=pltpu.SMEM)] if smem else []) + vmem(n_in)
    return pl.pallas_call(
        body,
        out_shape=outs,
        in_specs=in_specs,
        out_specs=vmem(len(outs)),
        scratch_shapes=[pltpu.VMEM(s, F32) for s in scratch],
        name=name,
        interpret=INTERPRET,
        compiler_params=pltpu.CompilerParams(vmem_limit_bytes=VMEM_LIMIT),
    )


INTERPRET = False
VMEM_LIMIT = 16 * 2**20


def pairs(n_gx, n_gy, axis, odd):
    count = n_gx if axis == 0 else n_gy
    result = []
    for i in range(n_gx):
        for j in range(n_gy):
            here = i if axis == 0 else j
            there = ((here + odd) ^ 1) - odd
            if 0 <= there < count:
                target = (there, j) if axis == 0 else (i, there)
                result.append((i * n_gy + j, target[0] * n_gy + target[1]))
    return result


def solution(mesh):
    n_gx, n_gy = mesh.shape["gx"], mesh.shape["gy"]

    def swap(a, b, axis):
        return (
            lax.ppermute(a, AX, pairs(n_gx, n_gy, axis, 0)),
            lax.ppermute(b, AX, pairs(n_gx, n_gy, axis, 1)),
        )

    box = sds(BX, ROWS, CZ)
    half = sds(BX // 2, ROWS, CZ)
    quarter = sds(BX // 4, ROWS, CZ)
    wide = sds(WX, ROWS, CZ)
    band = sds(YBAND, ROWS, CZ)
    yband = sds(YROWS, CZ)
    own = sds(CX, ROWS, CZ)
    coarse = [half.shape, half.shape, quarter.shape, quarter.shape]

    def on_device(right_side, shift):
        gx, gy = lax.axis_index("gx"), lax.axis_index("gy")
        idx = jnp.stack(
            [gx % 2, gy % 2]
            + [(c).astype(jnp.int32) for c in (gx == 0, gx == n_gx - 1, gy == 0, gy == n_gy - 1)]
        )

        def exchange_y(v, xa, xb):
            return swap(
                *call(
                    pack_y_kernel, "pack_y", 3, [yband, yband], [(WX, 16, CZ), (2, YROWS, CZ)]
                )(idx, v, xa, xb),
                1,
            )

        first = sds(2, 2, CY, CZ)
        xa, xb = swap(*call(pack_x_kernel, "pack_x", 2, [first, first])(idx, right_side, shift), 0)
        strip = sds(IROWS, CZ)
        rbox, sbox, ya, yb = call(
            box_kernel, "box", 4, [box, box, strip, strip], [(2, IROWS, CZ)]
        )(idx, right_side, shift, xa, xb)
        ya, yb = swap(ya, yb, 1)
        r0, v, xa, xb, *coefs = call(
            first_kernel,
            "first",
            4,
            [box, wide, band, band, box, box, half, half, quarter],
            [(2, IROWS, CZ), box.shape, half.shape] + coarse,
        )(idx, rbox, sbox, ya, yb)
        residuals, images = [r0], []
        for step in range(2):
            xa, xb = swap(xa, xb, 0)
            ya, yb = exchange_y(v, xa, xb)
            z, r, v, xa, xb = call(
                next_kernel,
                "next",
                11,
                [own, box, wide, band, band],
                [wide.shape, (2, YROWS, CZ)] + coarse,
            )(idx, v, xa, xb, ya, yb, residuals[-1], *coefs)
            images.append(z)
            residuals.append(r)
        xa, xb = swap(xa, xb, 0)
        ya, yb = exchange_y(v, xa, xb)
        z2, u2, sums = call(
            dots_kernel,
            "dots",
            11,
            [own, own, sds(n_gx * n_gy, CZ)],
            [wide.shape, (2, YROWS, CZ)],
        )(idx, v, xa, xb, ya, yb, coefs[0], *images, *residuals)
        gathered = lax.all_to_all(sums, AX, 0, 0, tiled=True)
        x, r = call(
            final_kernel, "final", 8, [sds(CX, CY, CZ), sds(CX, CY, CZ)], smem=False
        )(gathered, *images, z2, *residuals, u2)
        return x, r

    spec = P("gx", "gy", None)
    return jax.shard_map(
        on_device, mesh=mesh, in_specs=(spec, spec), out_specs=(spec, spec), check_vma=False
    )
```

```python
import jax
import jax.numpy as jnp
from jax import lax
from jax.experimental import pallas as pl
from jax.experimental.pallas import tpu as pltpu
from jax.sharding import PartitionSpec as P


STEP = 0.5
RELAX = 0.7
CENTER = 26.0
AX = ("gx", "gy")
CX, CY, CZ = 16, 32, 128
ROWS = 40
BX = CX + 4
WX = CX + 6
F32 = jnp.float32
IROWS = 80


def place():
    gx, gy = lax.axis_index("gx"), lax.axis_index("gy")
    ends = (gx == 0, gx == lax.axis_size("gx") - 1, gy == 0, gy == lax.axis_size("gy") - 1)
    return [gx & 1, gy & 1] + [jnp.where(end, 1, 0) for end in ends]


def sds(*shape):
    return jax.ShapeDtypeStruct(shape, F32)


def lanes():
    return lax.broadcasted_iota(jnp.int32, (ROWS, CZ), 1)


def rows():
    return lax.broadcasted_iota(jnp.int32, (ROWS, CZ), 0)


def zy_sum(p, sh):
    lane = lanes()
    zs = p + jnp.where(lane >= sh, pltpu.roll(p, sh, 1), 0.0)
    zs = zs + jnp.where(lane < CZ - sh, pltpu.roll(p, CZ - sh, 1), 0.0)
    return zs + pltpu.roll(zs, sh, 0) + pltpu.roll(zs, ROWS - sh, 0)


def band_matrix(terms, sh):
    at = lax.broadcasted_iota(jnp.int32, (terms * CZ, CZ), 0) & (CZ - 1)
    gap = jnp.abs(at - lax.broadcasted_iota(jnp.int32, (terms * CZ, CZ), 1))
    return jnp.where((gap == 0) | (gap == sh), 1.0, 0.0).astype(jnp.bfloat16)


def z_sums(planes, band):
    n = planes.shape[0]
    left = planes.reshape(n * ROWS, CZ)
    terms = []
    for _ in range(band.shape[0] // CZ):
        if terms:
            left = left - terms[-1].astype(F32)
        terms.append(left.astype(jnp.bfloat16))
    sums = jnp.dot(jnp.concatenate(terms, axis=1), band[...], preferred_element_type=F32)
    return sums.reshape(n, ROWS, CZ)


def wide_stencil(n, e, band, emit):
    sums = z_sums(e[...], band)

    def y_sum(x):
        zs = sums[x]
        return zs + pltpu.roll(zs, 1, 0) + pltpu.roll(zs, ROWS - 1, 0)

    prev, cur = None, y_sum(0)
    for x in range(n):
        nxt = y_sum(x + 1) if x + 1 < n else None
        total = cur
        if prev is not None:
            total = total + prev
        if nxt is not None:
            total = total + nxt
        emit(x, total)
        prev, cur = cur, nxt


def stencil(n, sh, load, emit):
    prev = None
    cur = zy_sum(load(0), sh)
    for x in range(n):
        nxt = zy_sum(load(x + 1), sh) if x + 1 < n else None
        total = cur
        if prev is not None:
            total = total + prev
        if nxt is not None:
            total = total + nxt
        emit(x, total)
        prev, cur = cur, nxt


def pair_sum(a, level):
    sh = 2**level
    bit = ((rows() + 7) >> level) & 1
    a = a + jnp.where(bit == 0, pltpu.roll(a, ROWS - sh, 0), pltpu.roll(a, sh, 0))
    bit = (lanes() >> level) & 1
    return a + jnp.where(bit == 0, pltpu.roll(a, CZ - sh, 1), pltpu.roll(a, sh, 1))


def smooth0(n, e, g, w, band):
    def emit(x, total):
        here = e[x]
        e[x] = (1.0 - RELAX) * here + w[x] * (g[x] + (total - here))

    wide_stencil(n, e, band, emit)


def smooth(n, sh, e, g, w):
    def emit(x, total):
        here = e[x]
        e[x] = (1.0 - RELAX) * here + w[x] * (g[x] + (total - here))

    stencil(n, sh, lambda x: e[x], emit)


def restrict(n, level, e, g, dp1, g_next, band=None):
    held = []

    def emit(x, total):
        left = (g[x] + total) - dp1[x] * e[x]
        if x % 2 == 0:
            held.append(left)
        else:
            g_next[x // 2] = 0.5 * pair_sum(held.pop() + left, level)

    if band is None:
        stencil(n, 2**level, lambda x: e[x], emit)
    else:
        wide_stencil(n, e, band, emit)


def vcycle(e0, g0, dp1_0, w0, dp1_1, w1, w2, e1, g1, e2, g2, band):
    n0, n1, n2 = BX, BX // 2, BX // 4
    for x in range(n0):
        e0[x] = w0[x] * g0[x]
    smooth0(n0, e0, g0, w0, band)
    restrict(n0, 0, e0, g0, dp1_0, g1, band)
    for x in range(n1):
        e1[x] = w1[x] * g1[x]
    smooth(n1, 2, e1, g1, w1)
    restrict(n1, 1, e1, g1, dp1_1, g2)
    for x in range(n2):
        e2[x] = w2[x] * g2[x]
    for _ in range(3):
        smooth(n2, 4, e2, g2, w2)
    for x in range(n1):
        e1[x] = e1[x] + e2[x // 2]
    for _ in range(2):
        smooth(n1, 2, e1, g1, w1)
    for x in range(n0):
        e0[x] = e0[x] + e1[x // 2]
    for _ in range(2):
        smooth0(n0, e0, g0, w0, band)


def send_x(idx, v, out_a, out_b):
    width = out_a.shape[0]
    low, high = 1, BX + 1 - width
    out_a[...] = v[pl.ds(jnp.where(idx[0] == 0, high, low), width)]
    out_b[...] = v[pl.ds(jnp.where(idx[0] == 0, low, high), width)]


def partner_b(idx, in_b):
    return jnp.where((idx[2] + idx[3]) == 0, in_b[idx[0]], 0.0)


def add_x(idx, w, in_a, in_b):
    width = in_a.shape[0]
    low, high = 5 - width, CX + 1
    a = jnp.where(idx[0] == 0, high, low)
    b = jnp.where(idx[0] == 0, low, high)
    w[pl.ds(a, width)] = w[pl.ds(a, width)] + in_a[...]
    w[pl.ds(b, width)] = w[pl.ds(b, width)] + partner_b(idx, in_b)


def pack_x_kernel(idx, r, s, out_a, out_b, sems):
    a = jnp.where(idx[0] == 0, CX - 2, 0)
    b = jnp.where(idx[0] == 0, 0, CX - 2)
    copies = [
        pltpu.make_async_copy(src.at[pl.ds(first, 2)], out.at[k], sems.at[2 * k + n])
        for k, src in enumerate((r, s))
        for n, (first, out) in enumerate(((a, out_a), (b, out_b)))
    ]
    for copy in copies:
        copy.start()
    for copy in copies:
        copy.wait()


def box_kernel(idx, r, s, in_a, in_b, rbox, sbox, out_a, out_b, pack):
    even = idx[0] == 0
    a = jnp.where(even, CX + 2, 0)
    b = jnp.where(even, 0, CX + 2)
    from_b = partner_b(idx, in_b)
    for k, (src, dst) in enumerate(((r, rbox), (s, sbox))):
        dst[...] = jnp.zeros_like(dst)
        for x in range(CX):
            dst[x + 2, 3 : 3 + CY, :] = src[x]
        for x in range(2):
            dst[a + x, 3 : 3 + CY, :] = in_a[k, x]
            dst[b + x, 3 : 3 + CY, :] = from_b[k, x]
        for x in range(BX):
            pack[0, 4 * x + 2 * k : 4 * x + 2 * k + 2, :] = dst[x, 3:5, :]
            pack[1, 4 * x + 2 * k : 4 * x + 2 * k + 2, :] = dst[x, 33:35, :]
    up = jnp.where(idx[1] == 0, 1, 0)
    out_a[...] = pack[up]
    out_b[...] = pack[1 - up]


def first_kernel(
    idx, rin, sin, in_a, in_b,
    r0, v, out_a, out_b, dp1_0, w0, dp1_1, w1, w2,
    got, s0, s1, e1, g1, e2, g2, band,
):
    up = jnp.where(idx[1] == 0, 1, 0)
    got[up] = in_a[...]
    got[1 - up] = jnp.where((idx[4] + idx[5]) == 0, in_b[idx[1]], 0.0)
    row = rows()
    inside = (row >= 1) & (row < 37)
    for k, (src, dst) in enumerate(((rin, r0), (sin, s0))):
        dst[...] = src[...]
        for x in range(BX):
            dst[x, 1:3, :] = got[0, 4 * x + 2 * k : 4 * x + 2 * k + 2, :]
            dst[x, 35:37, :] = got[1, 4 * x + 2 * k : 4 * x + 2 * k + 2, :]

    def coefficients(n, scale, s, dp1, w):
        for x in range(n):
            d = CENTER + scale * s[x]
            if dp1 is not None:
                dp1[x] = d + 1.0
            w[x] = jnp.where(inside, RELAX / d, 0.0)

    coefficients(BX, 1.0, s0, dp1_0, w0)
    for x in range(BX // 2):
        s1[x] = 0.125 * pair_sum(s0[2 * x] + s0[2 * x + 1], 0)
    coefficients(BX // 2, 4.0, s1, dp1_1, w1)
    for x in range(BX // 4):
        s0[x] = 0.125 * pair_sum(s1[2 * x] + s1[2 * x + 1], 1)
    coefficients(BX // 4, 16.0, s0, None, w2)
    band[...] = band_matrix(2, 1)
    v[0] = jnp.zeros((ROWS, CZ), F32)
    v[WX - 1] = jnp.zeros((ROWS, CZ), F32)
    vcycle(v.at[pl.ds(1, BX)], r0, dp1_0, w0, dp1_1, w1, w2, e1, g1, e2, g2, band)
    send_x(idx, v, out_a, out_b)


def pack_y_kernel(idx, v, in_a, in_b, out_a, out_b, w, pack):
    width = in_a.shape[0]
    x0 = 5 - width
    for x in range(WX):
        w[x, 0:8, :] = v[x, 0:8, :]
        w[x, 8:16, :] = v[x, 32:40, :]
    a = jnp.where(idx[0] == 0, CX + 1, x0)
    b = jnp.where(idx[0] == 0, x0, CX + 1)
    from_b = partner_b(idx, in_b)
    for first, src in ((a, in_a), (b, from_b)):
        for x in range(width):
            w[first + x, 0:8, :] = w[first + x, 0:8, :] + src[x, 0:8, :]
            w[first + x, 8:16, :] = w[first + x, 8:16, :] + src[x, 32:40, :]
    pack[:, pack.shape[1] - 8 :, :] = jnp.zeros((2, 8, CZ), F32)
    for x in range(x0, WX - x0):
        at = width * (x - x0)
        pack[0, at : at + width, :] = w[x, 1 : 1 + width, :]
        pack[1, at : at + width, :] = w[x, 13 - width : 13, :]
    up = jnp.where(idx[1] == 0, 1, 0)
    out_a[...] = pack[up]
    out_b[...] = pack[1 - up]


def assemble(idx, w, v, xa, xb, ya, yb, got):
    width = xa.shape[0]
    x0 = 5 - width
    w[...] = v[...]
    add_x(idx, w, xa, xb)
    up = jnp.where(idx[1] == 0, 1, 0)
    got[up] = ya[...]
    got[1 - up] = jnp.where((idx[4] + idx[5]) == 0, yb[idx[1]], 0.0)
    row = rows()
    mask = jnp.where(((row >= 3) | (idx[4] == 0)) & ((row < 3 + CY) | (idx[5] == 0)), 1.0, 0.0)
    for x in range(x0, WX - x0):
        at = width * (x - x0)
        w[x, x0:5, :] = w[x, x0:5, :] + got[0, at : at + width, :]
        w[x, 33 : 33 + width, :] = w[x, 33 : 33 + width, :] + got[1, at : at + width, :]
        m = mask
        if x < 3:
            m = mask * jnp.where(idx[2] == 0, 1.0, 0.0)
        if x >= CX + 3:
            m = mask * jnp.where(idx[3] == 0, 1.0, 0.0)
        w[x] = w[x] * m


def box_mask(idx, x):
    row = rows()
    low = jnp.where(idx[4] == 0, 1, 3)
    high = jnp.where(idx[5] == 0, 37, 35)
    m = jnp.where((row >= low) & (row < high), 1.0, 0.0)
    if x < 2:
        m = m * jnp.where(idx[2] == 0, 1.0, 0.0)
    if x >= CX + 2:
        m = m * jnp.where(idx[3] == 0, 1.0, 0.0)
    return m


def next_kernel(
    idx, vin, xa, xb, ya, yb, rin, dp1_0, w0, dp1_1, w1, w2,
    z, r, v, out_a, out_b,
    w, got, e1, g1, e2, g2, band,
):
    assemble(idx, w, vin, xa, xb, ya, yb, got)
    z[...] = w[pl.ds(3, CX)]

    def emit(x, total):
        if 1 <= x <= BX:
            image = dp1_0[x - 1] * w[x] - total
            r[x - 1] = rin[x - 1] - (STEP * box_mask(idx, x - 1)) * image

    wide_stencil(WX, w, band_matrix(3, 1), emit)
    band[...] = band_matrix(2, 1)
    v[0] = jnp.zeros((ROWS, CZ), F32)
    v[WX - 1] = jnp.zeros((ROWS, CZ), F32)
    vcycle(v.at[pl.ds(1, BX)], r, dp1_0, w0, dp1_1, w1, w2, e1, g1, e2, g2, band)
    send_x(idx, v, out_a, out_b)


def lane_sums(values):
    lane = lax.broadcasted_iota(jnp.int32, (1, CZ), 1)
    out = jnp.zeros((1, CZ), F32)
    for k, s in enumerate(values):
        part = jnp.sum(jnp.sum(s, axis=0, keepdims=True), axis=1, keepdims=True)
        out = out + jnp.where(lane == k, part, 0.0)
    return out


def own_rows():
    row = rows()
    return jnp.where((row >= 3) & (row < 3 + CY), 1.0, 0.0)


def early_kernel(z0, z1, r0, r1, r2, sums):
    own = own_rows()
    acc = [jnp.zeros((ROWS, CZ), F32) for _ in range(5)]
    for x in range(CX):
        a0, a1 = z0[x] * own, z1[x] * own
        b0, b1, b2 = r0[x + 2], r1[x + 2], r2[x + 2]
        terms = (a0 * b0, a0 * b1, a0 * b2, a1 * b1, a1 * b2)
        acc = [s + t for s, t in zip(acc, terms)]
    sums[...] = jnp.broadcast_to(lane_sums([acc[0] * 0.0] * 2 + acc), sums.shape)


def dots_kernel(idx, vin, xa, xb, ya, yb, dp1_0, r2, early, z2, u2, sums, w, got):
    assemble(idx, w, vin, xa, xb, ya, yb, got)
    own = own_rows()
    acc = [jnp.zeros((ROWS, CZ), F32) for _ in range(2)]

    def emit(x, total):
        if 3 <= x < 3 + CX:
            here = w[x]
            image = dp1_0[x - 1] * here - total
            z2[x - 3] = here
            u2[x - 3] = image
            here = here * own
            acc[0] = acc[0] + here * r2[x - 1]
            acc[1] = acc[1] + here * image

    wide_stencil(WX, w, band_matrix(3, 1), emit)
    sums[...] = jnp.broadcast_to(early[0:1, :] + lane_sums(acc), sums.shape)


def final_kernel(gathered, z0, z1, z2, r0, r1, r2, u2, x_out, r_out):
    row = jnp.sum(gathered[...], axis=0, keepdims=True)
    lane = lax.broadcasted_iota(jnp.int32, (1, CZ), 1)
    m22, h22, m00, m01, m02, m11, m12 = (
        jnp.sum(jnp.where(lane == k, row, 0.0), axis=1, keepdims=True) for k in range(7)
    )
    inv = 1.0 / STEP
    h00, h01, h02 = inv * (m00 - m01), inv * (m01 - m02), inv * (m02 - m12)
    h11, h12 = inv * (m11 - m12), inv * (m12 - m22)
    l10, l20 = h01 / h00, h02 / h00
    d1 = h11 - l10 * h01
    q = h12 - l10 * h02
    l21 = q / d1
    d2 = h22 - l20 * h02 - l21 * q
    y1 = m01 - l10 * m00
    y2 = m02 - l20 * m00 - l21 * y1
    c2 = y2 / d2
    c1 = y1 / d1 - l21 * c2
    c0 = m00 / h00 - l10 * c1 - l20 * c2
    f0, f1 = inv * c0, inv * c1
    for x in range(CX):
        xs = c0 * z0[x] + c1 * z1[x] + c2 * z2[x]
        b0, b1 = r0[x + 2], r1[x + 2]
        rs = b0 - f0 * (b0 - b1) - f1 * (b1 - r2[x + 2]) - c2 * u2[x]
        x_out[x] = xs[3 : 3 + CY, :]
        r_out[x] = rs[3 : 3 + CY, :]


def vmem(n):
    return [pl.BlockSpec(memory_space=pltpu.VMEM) for _ in range(n)]


def call(body, n_in, outs, scratch=(), smem=True, space=pltpu.VMEM):
    in_specs = [pl.BlockSpec(memory_space=space) for _ in range(n_in)]
    kernel = body
    if smem:

        def kernel(*refs):
            body(place(), *refs)

    return pl.pallas_call(
        kernel,
        out_shape=outs,
        in_specs=in_specs,
        out_specs=vmem(len(outs)),
        scratch_shapes=[pltpu.VMEM(s, F32) if isinstance(s, tuple) else s for s in scratch],
        interpret=INTERPRET,
        compiler_params=pltpu.CompilerParams(vmem_limit_bytes=VMEM_LIMIT),
    )


INTERPRET = False
VMEM_LIMIT = 16 * 2**20


def pairs(n_gx, n_gy, axis, odd):
    count = n_gx if axis == 0 else n_gy
    result = []
    for i in range(n_gx):
        for j in range(n_gy):
            here = i if axis == 0 else j
            there = ((here + odd) ^ 1) - odd
            if 0 <= there < count:
                target = (there, j) if axis == 0 else (i, there)
                result.append((i * n_gy + j, target[0] * n_gy + target[1]))
    return result


def solution(mesh):
    n_gx, n_gy = mesh.shape["gx"], mesh.shape["gy"]

    far = [[i * n_gy + j, i * n_gy + j + 1] for i in range(n_gx) for j in range(1, n_gy - 1, 2)]
    far += [[i * n_gy + j, (i + 1) * n_gy + j] for i in range(0, n_gx, 2) for j in (0, n_gy - 1)]
    neighbours = [[i * n_gy + j, (i + 1) * n_gy + j] for i in range(1, n_gx - 1, 2) for j in range(n_gy)]
    neighbours += [[i * n_gy + j, i * n_gy + j + 1] for i in (0, n_gx - 1) for j in range(0, n_gy, 2)]

    def swap_x(a, b):
        return (
            lax.ppermute(a, AX, pairs(n_gx, n_gy, 0, 0)),
            lax.all_gather(b, AX, axis_index_groups=neighbours),
        )

    def swap_y(a, b):
        a = lax.ppermute(a, AX, pairs(n_gx, n_gy, 1, 0))
        b = lax.all_gather(b, AX, axis_index_groups=far)
        return a, b

    box = sds(BX, ROWS, CZ)
    half = sds(BX // 2, ROWS, CZ)
    quarter = sds(BX // 4, ROWS, CZ)
    wide = sds(WX, ROWS, CZ)
    own = sds(CX, ROWS, CZ)
    band = pltpu.VMEM((2 * CZ, CZ), jnp.bfloat16)
    coarse = [half.shape, half.shape, quarter.shape, quarter.shape, band]

    def yrows(width):
        return -(-(CX - 4 + 2 * width) * width // 8) * 8

    def on_device(right_side, shift):
        def exchange(v, xa, xb):
            width = xa.shape[0]
            xa, xb = swap_x(xa, xb)
            size = yrows(width)
            ya, yb = call(
                pack_y_kernel, 3, [sds(size, CZ)] * 2, [(WX, 16, CZ), (2, size, CZ)]
            )(v, xa, xb)
            return (v, xa, xb) + swap_y(ya, yb)

        first = sds(2, 2, CY, CZ)
        xa, xb = call(
            pack_x_kernel, 2, [first, first], [pltpu.SemaphoreType.DMA((4,))], space=pltpu.HBM
        )(*(pltpu.with_memory_space_constraint(a, pltpu.HBM) for a in (right_side, shift)))
        xa, xb = swap_x(xa, xb)
        strip = sds(IROWS, CZ)
        rbox, sbox, ya, yb = call(
            box_kernel, 4, [box, box, strip, strip], [(2, IROWS, CZ)]
        )(right_side, shift, xa, xb)
        ya, yb = swap_y(ya, yb)
        r0, v, xa, xb, *coefs = call(
            first_kernel,
            4,
            [box, wide, sds(5, ROWS, CZ), sds(5, ROWS, CZ), box, box, half, half, quarter],
            [(2, IROWS, CZ), box.shape, half.shape] + coarse,
        )(rbox, sbox, ya, yb)
        residuals, images = [r0], []
        for width in (5, 3):
            z, r, v, xa, xb = call(
                next_kernel,
                11,
                [own, box, wide, sds(width, ROWS, CZ), sds(width, ROWS, CZ)],
                [wide.shape, (2, yrows(5), CZ)] + coarse,
            )(*exchange(v, xa, xb), residuals[-1], *coefs)
            images.append(z)
            residuals.append(r)
        early = call(early_kernel, 5, [sds(8, CZ)], smem=False)(*images, *residuals)[0]
        z2, u2, sums = call(
            dots_kernel, 8, [own, own, sds(n_gx * n_gy, CZ)], [wide.shape, (2, yrows(3), CZ)]
        )(*exchange(v, xa, xb), coefs[0], residuals[-1], early)
        gathered = lax.all_to_all(sums, AX, 0, 0, tiled=True)
        x, r = call(
            final_kernel, 8, [sds(CX, CY, CZ), sds(CX, CY, CZ)], smem=False
        )(gathered, *images, z2, *residuals, u2)
        return x, r

    spec = P("gx", "gy", None)
    return jax.shard_map(
        on_device, mesh=mesh, in_specs=(spec, spec), out_specs=(spec, spec), check_vma=False
    )
```

```python
import jax
import jax.numpy as jnp
import numpy as np
from jax import lax
from jax.experimental import pallas as pl
from jax.experimental.pallas import tpu as pltpu
from jax.sharding import PartitionSpec as P


STEP = 0.5
RELAX = 0.7
CENTER = 26.0
AX = ("gx", "gy")
CX, CY, CZ = 16, 32, 128
ROWS = 40
CROWS = 24
BX = CX + 4
WX = CX + 6
F32 = jnp.float32
IROWS = 80


def place():
    gx, gy = lax.axis_index("gx"), lax.axis_index("gy")
    ends = (gx == 0, gx == lax.axis_size("gx") - 1, gy == 0, gy == lax.axis_size("gy") - 1)
    return [gx & 1, gy & 1] + [jnp.where(end, 1, 0) for end in ends]


def sds(*shape):
    return jax.ShapeDtypeStruct(shape, F32)


def rows():
    return lax.broadcasted_iota(jnp.int32, (ROWS, CZ), 0)


def lane_matrix():
    gap = np.abs(np.arange(CZ)[:, None] - np.arange(CZ)[None, :])
    return np.tile(gap <= 1, (3, 1)).astype(jnp.bfloat16)


def z_sums(planes, band):
    n = planes.shape[0]
    left = planes.reshape(n * ROWS, CZ)
    terms = []
    for _ in range(band.shape[0] // CZ):
        if terms:
            left = left - terms[-1].astype(F32)
        terms.append(left.astype(jnp.bfloat16))
    sums = jnp.dot(jnp.concatenate(terms, axis=1), band[...], preferred_element_type=F32)
    return sums.reshape(n, ROWS, CZ)


def x_sums(n, plane, emit):
    planes = [plane(0)]
    pair = None
    for x in range(n):
        if x + 1 < n:
            planes.append(plane(x + 1))
        if x % 2 == 0:
            pair = planes[x] + planes[x + 1] if x + 1 < n else planes[x]
            total = pair + planes[x - 1] if x > 0 else pair
        else:
            total = pair + planes[x + 1] if x + 1 < n else pair
        emit(x, total)


def stencil(n, e, band, emit):
    sums = z_sums(e[...], band)

    def plane(x):
        zs = sums[x]
        return zs + pltpu.roll(zs, 1, 0) + pltpu.roll(zs, ROWS - 1, 0)

    x_sums(n, plane, emit)


def coarse_stencil(n, level, e, emit):
    sy, sz = 2 ** (level - 1), 2**level
    lane = lax.broadcasted_iota(jnp.int32, (CROWS, CZ), 1)

    def plane(x):
        p = e[x]
        zs = p + jnp.where(lane >= sz, pltpu.roll(p, sz, 1), 0.0)
        zs = zs + jnp.where(lane < CZ - sz, pltpu.roll(p, CZ - sz, 1), 0.0)
        return zs + pltpu.roll(zs, sy, 0) + pltpu.roll(zs, CROWS - sy, 0)

    x_sums(n, plane, emit)


def z_pairs(a, level):
    sh = 2**level
    bit = (lax.broadcasted_iota(jnp.int32, a.shape, 1) >> level) & 1
    return a + jnp.where(bit == 0, pltpu.roll(a, CZ - sh, 1), pltpu.roll(a, sh, 1))


def blocks1(tmp, x):
    a = tmp[x, pl.ds(1, CROWS, stride=2), :] + tmp[x, pl.ds(2, CROWS, stride=2), :]
    return z_pairs(a, 0)


def blocks2(a):
    bit = lax.broadcasted_iota(jnp.int32, (CROWS, CZ), 0) & 1
    a = a + jnp.where(bit == 0, pltpu.roll(a, CROWS - 1, 0), pltpu.roll(a, 1, 0))
    return z_pairs(a, 1)


def relaxed(e, g, w):
    def emit(x, total):
        e[x] = w[1, x] * e[x] + w[0, x] * (g[x] + total)

    return emit


def pairwise(e, g, dp1, use):
    held = []

    def emit(x, total):
        left = (g[x] + total) - dp1[x] * e[x]
        if x % 2 == 0:
            held.append(left)
        else:
            use(x // 2, held.pop() + left)

    return emit


def vcycle(e0, g0, dp1_0, w0, dp1_1, w1, w2, e1, g1, e2, g2, tmp, band):
    n0, n1, n2 = BX, BX // 2, BX // 4
    for x in range(n0):
        e0[x] = w0[0, x] * g0[x]
    stencil(n0, e0, band, relaxed(e0, g0, w0))

    def to_level1(k, left):
        tmp[k, 0:ROWS, :] = left
        g1[k] = 0.5 * blocks1(tmp, k)

    stencil(n0, e0, band, pairwise(e0, g0, dp1_0, to_level1))
    for x in range(n1):
        e1[x] = w1[0, x] * g1[x]
    coarse_stencil(n1, 1, e1, relaxed(e1, g1, w1))

    def to_level2(k, left):
        g2[k] = 0.5 * blocks2(left)

    coarse_stencil(n1, 1, e1, pairwise(e1, g1, dp1_1, to_level2))
    for x in range(n2):
        e2[x] = w2[0, x] * g2[x]
    for _ in range(3):
        coarse_stencil(n2, 2, e2, relaxed(e2, g2, w2))
    for x in range(n1):
        e1[x] = e1[x] + e2[x // 2]
    for _ in range(2):
        coarse_stencil(n1, 1, e1, relaxed(e1, g1, w1))
    for x in range(n1):
        tmp[x, pl.ds(1, CROWS, stride=2), :] = e1[x]
        tmp[x, pl.ds(2, CROWS, stride=2), :] = e1[x]
        tmp[x, 0:1, :] = jnp.zeros((1, CZ), F32)
    for x in range(n0):
        e0[x] = e0[x] + tmp[x // 2, 0:ROWS, :]
    for _ in range(2):
        stencil(n0, e0, band, relaxed(e0, g0, w0))


def clear_ends(tmp):
    for x in range(BX // 2):
        tmp[x, ROWS:, :] = jnp.zeros((16, CZ), F32)


def send_x(idx, v, out_a, out_b):
    width = out_a.shape[0]
    low, high = 1, BX + 1 - width
    out_a[...] = v[pl.ds(jnp.where(idx[0] == 0, high, low), width)]
    out_b[...] = v[pl.ds(jnp.where(idx[0] == 0, low, high), width)]


def partner_b(idx, in_b):
    return jnp.where((idx[2] + idx[3]) == 0, in_b[idx[0]], 0.0)


def add_x(idx, w, in_a, in_b):
    width = in_a.shape[0]
    low, high = 5 - width, CX + 1
    a = jnp.where(idx[0] == 0, high, low)
    b = jnp.where(idx[0] == 0, low, high)
    w[pl.ds(a, width)] = w[pl.ds(a, width)] + in_a[...]
    w[pl.ds(b, width)] = w[pl.ds(b, width)] + partner_b(idx, in_b)


def pack_x_kernel(idx, r, s, out_a, out_b, sems):
    a = jnp.where(idx[0] == 0, CX - 2, 0)
    b = jnp.where(idx[0] == 0, 0, CX - 2)
    copies = [
        pltpu.make_async_copy(src.at[pl.ds(first, 2)], out.at[k], sems.at[2 * k + n])
        for k, src in enumerate((r, s))
        for n, (first, out) in enumerate(((a, out_a), (b, out_b)))
    ]
    for copy in copies:
        copy.start()
    for copy in copies:
        copy.wait()


def box_kernel(idx, r, s, in_a, in_b, rbox, sbox, out_a, out_b, pack):
    even = idx[0] == 0
    a = jnp.where(even, CX + 2, 0)
    b = jnp.where(even, 0, CX + 2)
    from_b = partner_b(idx, in_b)
    for k, (src, dst) in enumerate(((r, rbox), (s, sbox))):
        dst[...] = jnp.zeros_like(dst)
        for x in range(CX):
            dst[x + 2, 3 : 3 + CY, :] = src[x]
        for x in range(2):
            dst[a + x, 3 : 3 + CY, :] = in_a[k, x]
            dst[b + x, 3 : 3 + CY, :] = from_b[k, x]
        for x in range(BX):
            pack[0, 4 * x + 2 * k : 4 * x + 2 * k + 2, :] = dst[x, 3:5, :]
            pack[1, 4 * x + 2 * k : 4 * x + 2 * k + 2, :] = dst[x, 33:35, :]
    up = jnp.where(idx[1] == 0, 1, 0)
    out_a[...] = pack[up]
    out_b[...] = pack[1 - up]


def first_kernel(
    idx, rin, sin, in_a, in_b, band,
    r0, v, out_a, out_b, dp1_0, w0, dp1_1, w1, w2,
    got, s0, s1, e1, g1, e2, g2, tmp,
):
    up = jnp.where(idx[1] == 0, 1, 0)
    got[up] = in_a[...]
    got[1 - up] = jnp.where((idx[4] + idx[5]) == 0, in_b[idx[1]], 0.0)
    for k, (src, dst) in enumerate(((rin, r0), (sin, s0))):
        dst[...] = src[...]
        for x in range(BX):
            dst[x, 1:3, :] = got[0, 4 * x + 2 * k : 4 * x + 2 * k + 2, :]
            dst[x, 35:37, :] = got[1, 4 * x + 2 * k : 4 * x + 2 * k + 2, :]

    def coefficients(x, scale, s, inside, dp1, w):
        d = CENTER + scale * s
        if dp1 is not None:
            dp1[x] = d + 1.0
        ratio = RELAX / d
        w[0, x] = jnp.where(inside, ratio, 0.0)
        w[1, x] = jnp.where(inside, (1.0 - RELAX) - ratio, 0.0)

    clear_ends(tmp)
    row = rows()
    for x in range(BX):
        coefficients(x, 1.0, s0[x], (row >= 1) & (row < 37), dp1_0, w0)
    inside = lax.broadcasted_iota(jnp.int32, (CROWS, CZ), 0) < (CY + 4) // 2
    for x in range(BX // 2):
        tmp[x, 0:ROWS, :] = s0[2 * x] + s0[2 * x + 1]
        s1[x] = 0.125 * blocks1(tmp, x)
        coefficients(x, 4.0, s1[x], inside, dp1_1, w1)
    for x in range(BX // 4):
        coefficients(x, 16.0, 0.125 * blocks2(s1[2 * x] + s1[2 * x + 1]), inside, None, w2)
    v[0] = jnp.zeros((ROWS, CZ), F32)
    v[WX - 1] = jnp.zeros((ROWS, CZ), F32)
    vcycle(v.at[pl.ds(1, BX)], r0, dp1_0, w0, dp1_1, w1, w2, e1, g1, e2, g2, tmp, band.at[pl.ds(0, 2 * CZ)])
    send_x(idx, v, out_a, out_b)


def pack_y_kernel(idx, v, in_a, in_b, out_a, out_b, w, pack):
    width = in_a.shape[0]
    x0 = 5 - width
    for x in range(WX):
        w[x, 0:8, :] = v[x, 0:8, :]
        w[x, 8:16, :] = v[x, 32:40, :]
    a = jnp.where(idx[0] == 0, CX + 1, x0)
    b = jnp.where(idx[0] == 0, x0, CX + 1)
    from_b = partner_b(idx, in_b)
    for first, src in ((a, in_a), (b, from_b)):
        for x in range(width):
            w[first + x, 0:8, :] = w[first + x, 0:8, :] + src[x, 0:8, :]
            w[first + x, 8:16, :] = w[first + x, 8:16, :] + src[x, 32:40, :]
    pack[:, pack.shape[1] - 8 :, :] = jnp.zeros((2, 8, CZ), F32)
    for x in range(x0, WX - x0):
        at = width * (x - x0)
        pack[0, at : at + width, :] = w[x, 1 : 1 + width, :]
        pack[1, at : at + width, :] = w[x, 13 - width : 13, :]
    up = jnp.where(idx[1] == 0, 1, 0)
    out_a[...] = pack[up]
    out_b[...] = pack[1 - up]


def assemble(idx, w, v, xa, xb, ya, yb, got):
    width = xa.shape[0]
    x0 = 5 - width
    w[...] = v[...]
    add_x(idx, w, xa, xb)
    up = jnp.where(idx[1] == 0, 1, 0)
    got[up] = ya[...]
    got[1 - up] = jnp.where((idx[4] + idx[5]) == 0, yb[idx[1]], 0.0)
    row = rows()
    mask = jnp.where(((row >= 3) | (idx[4] == 0)) & ((row < 3 + CY) | (idx[5] == 0)), 1.0, 0.0)
    for x in range(x0, WX - x0):
        at = width * (x - x0)
        w[x, x0:5, :] = w[x, x0:5, :] + got[0, at : at + width, :]
        w[x, 33 : 33 + width, :] = w[x, 33 : 33 + width, :] + got[1, at : at + width, :]
        m = mask
        if x < 3:
            m = mask * jnp.where(idx[2] == 0, 1.0, 0.0)
        if x >= CX + 3:
            m = mask * jnp.where(idx[3] == 0, 1.0, 0.0)
        w[x] = w[x] * m


def box_mask(idx, x):
    row = rows()
    low = jnp.where(idx[4] == 0, 1, 3)
    high = jnp.where(idx[5] == 0, 37, 35)
    m = jnp.where((row >= low) & (row < high), 1.0, 0.0)
    if x < 2:
        m = m * jnp.where(idx[2] == 0, 1.0, 0.0)
    if x >= CX + 2:
        m = m * jnp.where(idx[3] == 0, 1.0, 0.0)
    return m


def next_kernel(
    idx, vin, xa, xb, ya, yb, rin, dp1_0, w0, dp1_1, w1, w2, band,
    z, r, v, out_a, out_b,
    w, got, e1, g1, e2, g2, tmp,
):
    assemble(idx, w, vin, xa, xb, ya, yb, got)
    clear_ends(tmp)
    z[...] = w[pl.ds(3, CX)]

    def emit(x, total):
        if 1 <= x <= BX:
            image = dp1_0[x - 1] * w[x] - total
            r[x - 1] = rin[x - 1] - (STEP * box_mask(idx, x - 1)) * image

    stencil(WX, w, band, emit)
    v[0] = jnp.zeros((ROWS, CZ), F32)
    v[WX - 1] = jnp.zeros((ROWS, CZ), F32)
    vcycle(v.at[pl.ds(1, BX)], r, dp1_0, w0, dp1_1, w1, w2, e1, g1, e2, g2, tmp, band.at[pl.ds(0, 2 * CZ)])
    send_x(idx, v, out_a, out_b)


def lane_sums(values):
    lane = lax.broadcasted_iota(jnp.int32, (1, CZ), 1)
    out = jnp.zeros((1, CZ), F32)
    for k, s in enumerate(values):
        part = jnp.sum(jnp.sum(s, axis=0, keepdims=True), axis=1, keepdims=True)
        out = out + jnp.where(lane == k, part, 0.0)
    return out


def own_rows():
    row = rows()
    return jnp.where((row >= 3) & (row < 3 + CY), 1.0, 0.0)


def dots_kernel(idx, vin, xa, xb, ya, yb, dp1_0, z0, z1, r0, r1, r2, band, z2, u2, sums, w, got):
    assemble(idx, w, vin, xa, xb, ya, yb, got)
    own = own_rows()
    acc = [jnp.zeros((ROWS, CZ), F32) for _ in range(7)]

    def emit(x, total):
        if 3 <= x < 3 + CX:
            a2 = w[x]
            image = dp1_0[x - 1] * a2 - total
            z2[x - 3] = a2
            u2[x - 3] = image
            a0, a1, a2 = z0[x - 3] * own, z1[x - 3] * own, a2 * own
            b0, b1, b2 = r0[x - 1], r1[x - 1], r2[x - 1]
            terms = (a0 * b0, a0 * b1, a0 * b2, a1 * b1, a1 * b2, a2 * b2, a2 * image)
            acc[:] = [s + t for s, t in zip(acc, terms)]

    stencil(WX, w, band, emit)
    sums[...] = jnp.broadcast_to(lane_sums(acc), sums.shape)


def final_kernel(gathered, z0, z1, z2, r0, r1, r2, u2, x_out, r_out, x_part, r_part, sems):
    row = jnp.sum(gathered[...], axis=0, keepdims=True)
    lane = lax.broadcasted_iota(jnp.int32, (1, CZ), 1)
    m00, m01, m02, m11, m12, m22, h22 = (
        jnp.sum(jnp.where(lane == k, row, 0.0), axis=1, keepdims=True) for k in range(7)
    )
    inv = 1.0 / STEP
    h00, h01, h02 = inv * (m00 - m01), inv * (m01 - m02), inv * (m02 - m12)
    h11, h12 = inv * (m11 - m12), inv * (m12 - m22)
    l10, l20 = h01 / h00, h02 / h00
    d1 = h11 - l10 * h01
    q = h12 - l10 * h02
    l21 = q / d1
    d2 = h22 - l20 * h02 - l21 * q
    y1 = m01 - l10 * m00
    y2 = m02 - l20 * m00 - l21 * y1
    c2 = y2 / d2
    c1 = y1 / d1 - l21 * c2
    c0 = m00 / h00 - l10 * c1 - l20 * c2
    f0, f1 = inv * c0, inv * c1
    copies = []
    for x in range(CX):
        xs = c0 * z0[x] + c1 * z1[x] + c2 * z2[x]
        b0, b1 = r0[x + 2], r1[x + 2]
        rs = b0 - f0 * (b0 - b1) - f1 * (b1 - r2[x + 2]) - c2 * u2[x]
        x_part[x] = xs[3 : 3 + CY, :]
        r_part[x] = rs[3 : 3 + CY, :]
        if x % CHUNK == CHUNK - 1:
            part = pl.ds(x + 1 - CHUNK, CHUNK)
            for src, dst in ((x_part, x_out), (r_part, r_out)):
                copies.append(
                    pltpu.make_async_copy(src.at[part], dst.at[part], sems.at[len(copies)])
                )
                copies[-1].start()
    for copy in copies:
        copy.wait()


CHUNK = 4


def call(body, n_in, outs, scratch=(), smem=True, space=pltpu.VMEM, out=pltpu.VMEM):
    in_specs = [pl.BlockSpec(memory_space=space) for _ in range(n_in)]
    kernel = body
    if smem:

        def kernel(*refs):
            body(place(), *refs)

    return pl.pallas_call(
        kernel,
        out_shape=outs,
        in_specs=in_specs,
        out_specs=[pl.BlockSpec(memory_space=out) for _ in outs],
        scratch_shapes=[pltpu.VMEM(s, F32) if isinstance(s, tuple) else s for s in scratch],
        interpret=INTERPRET,
        compiler_params=pltpu.CompilerParams(vmem_limit_bytes=VMEM_LIMIT),
    )


INTERPRET = False
VMEM_LIMIT = 16 * 2**20


def pairs(n_gx, n_gy, axis, odd):
    count = n_gx if axis == 0 else n_gy
    result = []
    for i in range(n_gx):
        for j in range(n_gy):
            here = i if axis == 0 else j
            there = ((here + odd) ^ 1) - odd
            if 0 <= there < count:
                target = (there, j) if axis == 0 else (i, there)
                result.append((i * n_gy + j, target[0] * n_gy + target[1]))
    return result


def solution(mesh):
    n_gx, n_gy = mesh.shape["gx"], mesh.shape["gy"]

    far = [[i * n_gy + j, i * n_gy + j + 1] for i in range(n_gx) for j in range(1, n_gy - 1, 2)]
    far += [[i * n_gy + j, (i + 1) * n_gy + j] for i in range(0, n_gx, 2) for j in (0, n_gy - 1)]
    neighbours = [[i * n_gy + j, (i + 1) * n_gy + j] for i in range(1, n_gx - 1, 2) for j in range(n_gy)]
    neighbours += [[i * n_gy + j, i * n_gy + j + 1] for i in (0, n_gx - 1) for j in range(0, n_gy, 2)]

    def swap_x(a, b):
        return (
            lax.ppermute(a, AX, pairs(n_gx, n_gy, 0, 0)),
            lax.all_gather(b, AX, axis_index_groups=neighbours),
        )

    def swap_y(a, b):
        a = lax.ppermute(a, AX, pairs(n_gx, n_gy, 1, 0))
        b = lax.all_gather(b, AX, axis_index_groups=far)
        return a, b

    box = sds(BX, ROWS, CZ)
    half = sds(BX // 2, CROWS, CZ)
    quarter = sds(BX // 4, CROWS, CZ)
    weights = [sds(2, BX, ROWS, CZ), half, sds(2, BX // 2, CROWS, CZ), sds(2, BX // 4, CROWS, CZ)]
    wide = sds(WX, ROWS, CZ)
    own = sds(CX, ROWS, CZ)
    coarse = [half.shape, half.shape, quarter.shape, quarter.shape, (BX // 2, ROWS + 16, CZ)]

    def yrows(width):
        return -(-(CX - 4 + 2 * width) * width // 8) * 8

    def on_device(right_side, shift):
        def exchange(v, xa, xb):
            width = xa.shape[0]
            xa, xb = swap_x(xa, xb)
            size = yrows(width)
            ya, yb = call(pack_y_kernel, 3, [sds(size, CZ)] * 2, [(WX, 16, CZ), (2, size, CZ)])(v, xa, xb)
            return (v, xa, xb) + swap_y(ya, yb)

        matrix = jnp.asarray(lane_matrix())
        first = sds(2, 2, CY, CZ)
        xa, xb = call(
            pack_x_kernel, 2, [first, first], [pltpu.SemaphoreType.DMA((4,))], space=pltpu.HBM
        )(*(pltpu.with_memory_space_constraint(a, pltpu.HBM) for a in (right_side, shift)))
        xa, xb = swap_x(xa, xb)
        strip = sds(IROWS, CZ)
        rbox, sbox, ya, yb = call(box_kernel, 4, [box, box, strip, strip], [(2, IROWS, CZ)])(right_side, shift, xa, xb)
        ya, yb = swap_y(ya, yb)
        r0, v, xa, xb, *coefs = call(
            first_kernel,
            5,
            [box, wide, sds(5, ROWS, CZ), sds(5, ROWS, CZ), box] + weights,
            [(2, IROWS, CZ), box.shape, half.shape] + coarse,
        )(rbox, sbox, ya, yb, matrix)
        residuals, images = [r0], []
        for width in (5, 3):
            z, r, v, xa, xb = call(
                next_kernel,
                12,
                [own, box, wide, sds(width, ROWS, CZ), sds(width, ROWS, CZ)],
                [wide.shape, (2, yrows(5), CZ)] + coarse,
            )(*exchange(v, xa, xb), residuals[-1], *coefs, matrix)
            images.append(z)
            residuals.append(r)
        z2, u2, sums = call(
            dots_kernel, 12, [own, own, sds(n_gx * n_gy, CZ)], [wide.shape, (2, yrows(3), CZ)]
        )(*exchange(v, xa, xb), coefs[0], *images, *residuals, matrix)
        gathered = lax.all_to_all(sums, AX, 0, 0, tiled=True)
        x, r = call(
            final_kernel,
            8,
            [sds(CX, CY, CZ)] * 2,
            [(CX, CY, CZ), (CX, CY, CZ), pltpu.SemaphoreType.DMA((2 * CX // CHUNK,))],
            smem=False,
            out=pltpu.HBM,
        )(gathered, *images, z2, *residuals, u2)
        return x, r

    spec = P("gx", "gy", None)
    return jax.shard_map(
        on_device, mesh=mesh, in_specs=(spec, spec), out_specs=(spec, spec), check_vma=False
    )
```

```python
import jax
import jax.numpy as jnp
import numpy as np
from jax import lax
from jax.experimental import pallas as pl
from jax.experimental.pallas import tpu as pltpu
from jax.sharding import PartitionSpec as P


STEP = 0.5
RELAX = 0.7
CENTER = 26.0
AX = ("gx", "gy")
CX, CY, CZ = 16, 32, 128
ROWS = 40
CROWS = 24
BX = CX + 4
WX = CX + 6
F32 = jnp.float32
IROWS = 80


def place():
    gx, gy = lax.axis_index("gx"), lax.axis_index("gy")
    ends = (gx == 0, gx == lax.axis_size("gx") - 1, gy == 0, gy == lax.axis_size("gy") - 1)
    return [gx & 1, gy & 1] + [jnp.where(end, 1, 0) for end in ends]


def sds(*shape):
    return jax.ShapeDtypeStruct(shape, F32)


def rows():
    return lax.broadcasted_iota(jnp.int32, (ROWS, CZ), 0)


def lane_matrix():
    gap = np.abs(np.arange(CZ)[:, None] - np.arange(CZ)[None, :])
    return np.tile(gap <= 1, (3, 1)).astype(jnp.bfloat16)


def z_sums(planes, band):
    n = planes.shape[0]
    left = planes.reshape(n * ROWS, CZ)
    terms = []
    for _ in range(band.shape[0] // CZ):
        if terms:
            left = left - terms[-1].astype(F32)
        terms.append(left.astype(jnp.bfloat16))
    sums = jnp.dot(jnp.concatenate(terms, axis=1), band[...], preferred_element_type=F32)
    return sums.reshape(n, ROWS, CZ)


def x_sums(n, plane, emit):
    planes = [plane(0)]
    pair = None
    for x in range(n):
        if x + 1 < n:
            planes.append(plane(x + 1))
        if x % 2 == 0:
            pair = planes[x] + planes[x + 1] if x + 1 < n else planes[x]
            total = pair + planes[x - 1] if x > 0 else pair
        else:
            total = pair + planes[x + 1] if x + 1 < n else pair
        emit(x, total)


def stencil(n, e, band, emit):
    sums = z_sums(e[...], band)

    def plane(x):
        zs = sums[x]
        return zs + pltpu.roll(zs, 1, 0) + pltpu.roll(zs, ROWS - 1, 0)

    x_sums(n, plane, emit)


def coarse_stencil(n, level, e, emit):
    sy, sz = 2 ** (level - 1), 2**level
    lane = lax.broadcasted_iota(jnp.int32, (CROWS, CZ), 1)

    def plane(x):
        p = e[x]
        zs = p + jnp.where(lane >= sz, pltpu.roll(p, sz, 1), 0.0)
        zs = zs + jnp.where(lane < CZ - sz, pltpu.roll(p, CZ - sz, 1), 0.0)
        return zs + pltpu.roll(zs, sy, 0) + pltpu.roll(zs, CROWS - sy, 0)

    x_sums(n, plane, emit)


def z_pairs(a, level):
    sh = 2**level
    bit = (lax.broadcasted_iota(jnp.int32, a.shape, 1) >> level) & 1
    return a + jnp.where(bit == 0, pltpu.roll(a, CZ - sh, 1), pltpu.roll(a, sh, 1))


def blocks1(tmp, x):
    a = tmp[x, pl.ds(1, CROWS, stride=2), :] + tmp[x, pl.ds(2, CROWS, stride=2), :]
    return z_pairs(a, 0)


def blocks2(a):
    bit = lax.broadcasted_iota(jnp.int32, (CROWS, CZ), 0) & 1
    a = a + jnp.where(bit == 0, pltpu.roll(a, CROWS - 1, 0), pltpu.roll(a, 1, 0))
    return z_pairs(a, 1)


def relaxed(e, g, w):
    def emit(x, total):
        e[x] = w[1, x] * e[x] + w[0, x] * (g[x] + total)

    return emit


def pairwise(e, g, dp1, use):
    held = []

    def emit(x, total):
        left = (g[x] + total) - dp1[x] * e[x]
        if x % 2 == 0:
            held.append(left)
        else:
            use(x // 2, held.pop() + left)

    return emit


def vcycle(e0, g0, dp1_0, w0, dp1_1, w1, w2, e1, g1, e2, g2, tmp, band):
    n0, n1, n2 = BX, BX // 2, BX // 4
    for x in range(n0):
        e0[x] = w0[0, x] * g0[x]
    stencil(n0, e0, band, relaxed(e0, g0, w0))

    def to_level1(k, left):
        tmp[k, 0:ROWS, :] = left
        g1[k] = 0.5 * blocks1(tmp, k)

    stencil(n0, e0, band, pairwise(e0, g0, dp1_0, to_level1))
    for x in range(n1):
        e1[x] = w1[0, x] * g1[x]
    coarse_stencil(n1, 1, e1, relaxed(e1, g1, w1))

    def to_level2(k, left):
        g2[k] = 0.5 * blocks2(left)

    coarse_stencil(n1, 1, e1, pairwise(e1, g1, dp1_1, to_level2))
    for x in range(n2):
        e2[x] = w2[0, x] * g2[x]
    for _ in range(3):
        coarse_stencil(n2, 2, e2, relaxed(e2, g2, w2))
    for x in range(n1):
        e1[x] = e1[x] + e2[x // 2]
    for _ in range(2):
        coarse_stencil(n1, 1, e1, relaxed(e1, g1, w1))
    for x in range(n1):
        tmp[x, pl.ds(1, CROWS, stride=2), :] = e1[x]
        tmp[x, pl.ds(2, CROWS, stride=2), :] = e1[x]
        tmp[x, 0:1, :] = jnp.zeros((1, CZ), F32)
    for x in range(n0):
        e0[x] = e0[x] + tmp[x // 2, 0:ROWS, :]
    for _ in range(2):
        stencil(n0, e0, band, relaxed(e0, g0, w0))


def clear_ends(tmp):
    for x in range(BX // 2):
        tmp[x, ROWS:, :] = jnp.zeros((16, CZ), F32)


def send_x(idx, v, out_a, out_b):
    width = out_a.shape[0]
    low, high = 1, BX + 1 - width
    out_a[...] = v[pl.ds(jnp.where(idx[0] == 0, high, low), width)]
    out_b[...] = v[pl.ds(jnp.where(idx[0] == 0, low, high), width)]


def partner_b(idx, in_b):
    return jnp.where((idx[2] + idx[3]) == 0, in_b[idx[0]], 0.0)


def pack_x_kernel(idx, r, s, out_a, out_b, sems):
    a = jnp.where(idx[0] == 0, CX - 2, 0)
    b = jnp.where(idx[0] == 0, 0, CX - 2)
    copies = [
        pltpu.make_async_copy(src.at[pl.ds(first, 2)], out.at[k], sems.at[2 * k + n])
        for k, src in enumerate((r, s))
        for n, (first, out) in enumerate(((a, out_a), (b, out_b)))
    ]
    for copy in copies:
        copy.start()
    for copy in copies:
        copy.wait()


def box_kernel(idx, r, s, in_a, in_b, rbox, sbox, out_a, out_b, pack):
    even = idx[0] == 0
    a = jnp.where(even, CX + 2, 0)
    b = jnp.where(even, 0, CX + 2)
    from_b = partner_b(idx, in_b)
    for k, (src, dst) in enumerate(((r, rbox), (s, sbox))):
        dst[...] = jnp.zeros_like(dst)
        for x in range(CX):
            dst[x + 2, 3 : 3 + CY, :] = src[x]
        for x in range(2):
            dst[a + x, 3 : 3 + CY, :] = in_a[k, x]
            dst[b + x, 3 : 3 + CY, :] = from_b[k, x]
        for x in range(BX):
            pack[0, 4 * x + 2 * k : 4 * x + 2 * k + 2, :] = dst[x, 3:5, :]
            pack[1, 4 * x + 2 * k : 4 * x + 2 * k + 2, :] = dst[x, 33:35, :]
    up = jnp.where(idx[1] == 0, 1, 0)
    out_a[...] = pack[up]
    out_b[...] = pack[1 - up]


def first_kernel(
    idx, rin, sin, in_a, in_b, band,
    r0, v, out_a, out_b, dp1_0, w0, dp1_1, w1, w2,
    got, s0, s1, e1, g1, e2, g2, tmp,
):
    up = jnp.where(idx[1] == 0, 1, 0)
    got[up] = in_a[...]
    got[1 - up] = jnp.where((idx[4] + idx[5]) == 0, in_b[idx[1]], 0.0)
    for k, (src, dst) in enumerate(((rin, r0), (sin, s0))):
        dst[...] = src[...]
        for x in range(BX):
            dst[x, 1:3, :] = got[0, 4 * x + 2 * k : 4 * x + 2 * k + 2, :]
            dst[x, 35:37, :] = got[1, 4 * x + 2 * k : 4 * x + 2 * k + 2, :]

    def coefficients(x, scale, s, inside, dp1, w):
        d = CENTER + scale * s
        if dp1 is not None:
            dp1[x] = d + 1.0
        ratio = RELAX / d
        w[0, x] = jnp.where(inside, ratio, 0.0)
        w[1, x] = jnp.where(inside, (1.0 - RELAX) - ratio, 0.0)

    clear_ends(tmp)
    row = rows()
    for x in range(BX):
        coefficients(x, 1.0, s0[x], (row >= 1) & (row < 37), dp1_0, w0)
    inside = lax.broadcasted_iota(jnp.int32, (CROWS, CZ), 0) < (CY + 4) // 2
    for x in range(BX // 2):
        tmp[x, 0:ROWS, :] = s0[2 * x] + s0[2 * x + 1]
        s1[x] = 0.125 * blocks1(tmp, x)
        coefficients(x, 4.0, s1[x], inside, dp1_1, w1)
    for x in range(BX // 4):
        coefficients(x, 16.0, 0.125 * blocks2(s1[2 * x] + s1[2 * x + 1]), inside, None, w2)
    v[0] = jnp.zeros((ROWS, CZ), F32)
    v[WX - 1] = jnp.zeros((ROWS, CZ), F32)
    vcycle(v.at[pl.ds(1, BX)], r0, dp1_0, w0, dp1_1, w1, w2, e1, g1, e2, g2, tmp, band.at[pl.ds(0, 2 * CZ)])
    send_x(idx, v, out_a, out_b)


def pack_y_kernel(idx, v, in_a, in_b, out_a, out_b, w, pack):
    width = in_a.shape[0]
    x0 = 5 - width
    for x in range(WX):
        w[x, 0:8, :] = v[x, 0:8, :]
        w[x, 8:16, :] = v[x, 32:40, :]
    a = jnp.where(idx[0] == 0, CX + 1, x0)
    b = jnp.where(idx[0] == 0, x0, CX + 1)
    from_b = partner_b(idx, in_b)
    for first, src in ((a, in_a), (b, from_b)):
        for x in range(width):
            w[first + x, 0:8, :] = w[first + x, 0:8, :] + src[x, 0:8, :]
            w[first + x, 8:16, :] = w[first + x, 8:16, :] + src[x, 32:40, :]
    pack[:, pack.shape[1] - 8 :, :] = jnp.zeros((2, 8, CZ), F32)
    for x in range(x0, WX - x0):
        at = width * (x - x0)
        pack[0, at : at + width, :] = w[x, 1 : 1 + width, :]
        pack[1, at : at + width, :] = w[x, 13 - width : 13, :]
    up = jnp.where(idx[1] == 0, 1, 0)
    out_a[...] = pack[up]
    out_b[...] = pack[1 - up]


def assemble(idx, w, v, xa, xb, ya, yb, got):
    width = xa.shape[0]
    size = ya.shape[0]
    x0 = 5 - width
    even = idx[0] == 0
    from_a = idx[1] == 1
    far = jnp.where((idx[4] + idx[5]) == 0, yb[idx[1]], 0.0)
    near = ya[...]
    got[0, 8 : 8 + size, :] = jnp.where(from_a, near, far)
    got[1, 8 : 8 + size, :] = jnp.where(from_a, far, near)
    inner = (idx[2] + idx[3]) == 0
    row = lax.broadcasted_iota(jnp.int32, (8, CZ), 0)
    low_mask = jnp.where((row >= 3) | (idx[4] == 0), 1.0, 0.0)
    high_mask = jnp.where((row < 3) | (idx[5] == 0), 1.0, 0.0)
    for x in range(WX):
        plane = v[x]
        if x0 <= x < 5 or CX + 1 <= x < WX - x0:
            k = x - x0 if x < 5 else x - (CX + 1)
            upper = jnp.where(inner, xb[idx[0], k], 0.0)
            plane = plane + jnp.where(even == (x > 5), xa[k], upper)
        low, middle, high = plane[0:8], plane[8:32], plane[32:40]
        if x0 <= x < WX - x0:
            at = 8 + width * (x - x0)
            take = (row >= x0) & (row < 5)
            low = low + jnp.where(take, got[0, at - x0 : at - x0 + 8, :], 0.0)
            take = (row >= 1) & (row < 1 + width)
            high = high + jnp.where(take, got[1, at - 1 : at + 7, :], 0.0)
        low, high = low * low_mask, high * high_mask
        plane = jnp.concatenate([low, middle, high], axis=0)
        if x < 3:
            plane = plane * jnp.where(idx[2] == 0, 1.0, 0.0)
        if x >= CX + 3:
            plane = plane * jnp.where(idx[3] == 0, 1.0, 0.0)
        w[x] = plane


def box_mask(idx, x):
    row = rows()
    low = jnp.where(idx[4] == 0, 1, 3)
    high = jnp.where(idx[5] == 0, 37, 35)
    m = jnp.where((row >= low) & (row < high), 1.0, 0.0)
    if x < 2:
        m = m * jnp.where(idx[2] == 0, 1.0, 0.0)
    if x >= CX + 2:
        m = m * jnp.where(idx[3] == 0, 1.0, 0.0)
    return m


def next_kernel(
    idx, vin, xa, xb, ya, yb, rin, dp1_0, w0, dp1_1, w1, w2, band,
    z, r, v, out_a, out_b,
    w, got, e1, g1, e2, g2, tmp,
):
    assemble(idx, w, vin, xa, xb, ya, yb, got)
    clear_ends(tmp)

    def emit(x, total):
        if 1 <= x <= BX:
            here = w[x]
            image = dp1_0[x - 1] * here - total
            if 3 <= x < 3 + CX:
                z[x - 3] = here
            r[x - 1] = rin[x - 1] - (STEP * box_mask(idx, x - 1)) * image

    stencil(WX, w, band, emit)
    v[0] = jnp.zeros((ROWS, CZ), F32)
    v[WX - 1] = jnp.zeros((ROWS, CZ), F32)
    vcycle(v.at[pl.ds(1, BX)], r, dp1_0, w0, dp1_1, w1, w2, e1, g1, e2, g2, tmp, band.at[pl.ds(0, 2 * CZ)])
    send_x(idx, v, out_a, out_b)


def lane_sums(values):
    lane = lax.broadcasted_iota(jnp.int32, (1, CZ), 1)
    out = jnp.zeros((1, CZ), F32)
    for k, s in enumerate(values):
        part = jnp.sum(jnp.sum(s, axis=0, keepdims=True), axis=1, keepdims=True)
        out = out + jnp.where(lane == k, part, 0.0)
    return out


def own_rows():
    row = rows()
    return jnp.where((row >= 3) & (row < 3 + CY), 1.0, 0.0)


def dots_kernel(idx, vin, xa, xb, ya, yb, dp1_0, z0, z1, r0, r1, r2, band, z2, u2, sums, w, got):
    assemble(idx, w, vin, xa, xb, ya, yb, got)
    acc = [jnp.zeros((ROWS, CZ), F32) for _ in range(7)]

    def emit(x, total):
        if 3 <= x < 3 + CX:
            a2 = w[x]
            image = dp1_0[x - 1] * a2 - total
            z2[x - 3] = a2
            u2[x - 3] = image
            a0, a1 = z0[x - 3], z1[x - 3]
            b0, b1, b2 = r0[x - 1], r1[x - 1], r2[x - 1]
            terms = (a0 * b0, a0 * b1, a0 * b2, a1 * b1, a1 * b2, a2 * b2, a2 * image)
            acc[:] = [s + t for s, t in zip(acc, terms)]

    stencil(WX, w, band, emit)
    own = own_rows()
    sums[...] = jnp.broadcast_to(lane_sums([s * own for s in acc]), sums.shape)


def final_kernel(gathered, z0, z1, z2, r0, r1, r2, u2, x_out, r_out, x_part, r_part, sems):
    row = jnp.sum(gathered[...], axis=0, keepdims=True)
    lane = lax.broadcasted_iota(jnp.int32, (1, CZ), 1)
    m00, m01, m02, m11, m12, m22, h22 = (
        jnp.sum(jnp.where(lane == k, row, 0.0), axis=1, keepdims=True) for k in range(7)
    )
    inv = 1.0 / STEP
    h00, h01, h02 = inv * (m00 - m01), inv * (m01 - m02), inv * (m02 - m12)
    h11, h12 = inv * (m11 - m12), inv * (m12 - m22)
    l10, l20 = h01 / h00, h02 / h00
    d1 = h11 - l10 * h01
    q = h12 - l10 * h02
    l21 = q / d1
    d2 = h22 - l20 * h02 - l21 * q
    y1 = m01 - l10 * m00
    y2 = m02 - l20 * m00 - l21 * y1
    c2 = y2 / d2
    c1 = y1 / d1 - l21 * c2
    c0 = m00 / h00 - l10 * c1 - l20 * c2
    f0, f1 = inv * c0, inv * c1
    copies = []
    for x in range(CX):
        xs = c0 * z0[x] + c1 * z1[x] + c2 * z2[x]
        b0, b1 = r0[x + 2], r1[x + 2]
        rs = b0 - f0 * (b0 - b1) - f1 * (b1 - r2[x + 2]) - c2 * u2[x]
        x_part[x] = xs[3 : 3 + CY, :]
        r_part[x] = rs[3 : 3 + CY, :]
        if x % CHUNK == CHUNK - 1:
            part = pl.ds(x + 1 - CHUNK, CHUNK)
            for src, dst in ((x_part, x_out), (r_part, r_out)):
                copies.append(
                    pltpu.make_async_copy(src.at[part], dst.at[part], sems.at[len(copies)])
                )
                copies[-1].start()
    for copy in copies:
        copy.wait()


CHUNK = 4


def call(body, n_in, outs, scratch=(), smem=True, space=pltpu.VMEM, out=pltpu.VMEM):
    in_specs = [pl.BlockSpec(memory_space=space) for _ in range(n_in)]
    kernel = body
    if smem:

        def kernel(*refs):
            body(place(), *refs)

    return pl.pallas_call(
        kernel,
        out_shape=outs,
        in_specs=in_specs,
        out_specs=[pl.BlockSpec(memory_space=out) for _ in outs],
        scratch_shapes=[pltpu.VMEM(s, F32) if isinstance(s, tuple) else s for s in scratch],
        interpret=INTERPRET,
        compiler_params=pltpu.CompilerParams(vmem_limit_bytes=VMEM_LIMIT),
    )


INTERPRET = False
VMEM_LIMIT = 16 * 2**20


def pairs(n_gx, n_gy, axis, odd):
    count = n_gx if axis == 0 else n_gy
    result = []
    for i in range(n_gx):
        for j in range(n_gy):
            here = i if axis == 0 else j
            there = ((here + odd) ^ 1) - odd
            if 0 <= there < count:
                target = (there, j) if axis == 0 else (i, there)
                result.append((i * n_gy + j, target[0] * n_gy + target[1]))
    return result


def solution(mesh):
    n_gx, n_gy = mesh.shape["gx"], mesh.shape["gy"]

    far = [[i * n_gy + j, i * n_gy + j + 1] for i in range(n_gx) for j in range(1, n_gy - 1, 2)]
    far += [[i * n_gy + j, (i + 1) * n_gy + j] for i in range(0, n_gx, 2) for j in (0, n_gy - 1)]
    neighbours = [[i * n_gy + j, (i + 1) * n_gy + j] for i in range(1, n_gx - 1, 2) for j in range(n_gy)]
    neighbours += [[i * n_gy + j, i * n_gy + j + 2] for i in (0, n_gx - 1) for j in range(n_gy) if j % 4 < 2]

    def swap_x(a, b):
        return (
            lax.ppermute(a, AX, pairs(n_gx, n_gy, 0, 0)),
            lax.all_gather(b, AX, axis_index_groups=neighbours),
        )

    def swap_y(a, b):
        a = lax.ppermute(a, AX, pairs(n_gx, n_gy, 1, 0))
        b = lax.all_gather(b, AX, axis_index_groups=far)
        return a, b

    box = sds(BX, ROWS, CZ)
    half = sds(BX // 2, CROWS, CZ)
    quarter = sds(BX // 4, CROWS, CZ)
    weights = [sds(2, BX, ROWS, CZ), half, sds(2, BX // 2, CROWS, CZ), sds(2, BX // 4, CROWS, CZ)]
    wide = sds(WX, ROWS, CZ)
    own = sds(CX, ROWS, CZ)
    coarse = [half.shape, half.shape, quarter.shape, quarter.shape, (BX // 2, ROWS + 16, CZ)]

    def yrows(width):
        return -(-(CX - 4 + 2 * width) * width // 8) * 8

    def on_device(right_side, shift):
        def exchange(v, xa, xb):
            width = xa.shape[0]
            xa, xb = swap_x(xa, xb)
            size = yrows(width)
            ya, yb = call(pack_y_kernel, 3, [sds(size, CZ)] * 2, [(WX, 16, CZ), (2, size, CZ)])(v, xa, xb)
            return (v, xa, xb) + swap_y(ya, yb)

        matrix = jnp.asarray(lane_matrix())
        first = sds(2, 2, CY, CZ)
        xa, xb = call(
            pack_x_kernel, 2, [first, first], [pltpu.SemaphoreType.DMA((4,))], space=pltpu.HBM
        )(*(pltpu.with_memory_space_constraint(a, pltpu.HBM) for a in (right_side, shift)))
        xa, xb = swap_x(xa, xb)
        strip = sds(IROWS, CZ)
        rbox, sbox, ya, yb = call(box_kernel, 4, [box, box, strip, strip], [(2, IROWS, CZ)])(right_side, shift, xa, xb)
        ya, yb = swap_y(ya, yb)
        r0, v, xa, xb, *coefs = call(
            first_kernel,
            5,
            [box, wide, sds(5, ROWS, CZ), sds(5, ROWS, CZ), box] + weights,
            [(2, IROWS, CZ), box.shape, half.shape] + coarse,
        )(rbox, sbox, ya, yb, matrix)
        residuals, images = [r0], []
        for width in (5, 3):
            z, r, v, xa, xb = call(
                next_kernel,
                12,
                [own, box, wide, sds(width, ROWS, CZ), sds(width, ROWS, CZ)],
                [wide.shape, (2, yrows(5) + 16, CZ)] + coarse,
            )(*exchange(v, xa, xb), residuals[-1], *coefs, matrix)
            images.append(z)
            residuals.append(r)
        z2, u2, sums = call(
            dots_kernel, 12, [own, own, sds(n_gx * n_gy, CZ)], [wide.shape, (2, yrows(3) + 16, CZ)]
        )(*exchange(v, xa, xb), coefs[0], *images, *residuals, matrix)
        gathered = lax.all_to_all(sums, AX, 0, 0, tiled=True)
        x, r = call(
            final_kernel,
            8,
            [sds(CX, CY, CZ)] * 2,
            [(CX, CY, CZ), (CX, CY, CZ), pltpu.SemaphoreType.DMA((2 * CX // CHUNK,))],
            smem=False,
            out=pltpu.HBM,
        )(gathered, *images, z2, *residuals, u2)
        return x, r

    spec = P("gx", "gy", None)
    return jax.shard_map(
        on_device, mesh=mesh, in_specs=(spec, spec), out_specs=(spec, spec), check_vma=False
    )
```

```python
import jax
import jax.numpy as jnp
import numpy as np
from jax import lax
from jax.experimental import pallas as pl
from jax.experimental.pallas import tpu as pltpu
from jax.sharding import PartitionSpec as P


STEP = 0.5
RELAX = 0.7
CENTER = 26.0
AX = ("gx", "gy")
CX, CY, CZ = 16, 32, 128
ROWS = 40
CROWS = 24
BX = CX + 4
WX = CX + 6
F32 = jnp.float32
IROWS = 80


def place():
    gx, gy = lax.axis_index("gx"), lax.axis_index("gy")
    ends = (gx == 0, gx == lax.axis_size("gx") - 1, gy == 0, gy == lax.axis_size("gy") - 1)
    return [gx & 1, gy & 1] + [jnp.where(end, 1, 0) for end in ends]


def sds(*shape):
    return jax.ShapeDtypeStruct(shape, F32)


def rows():
    return lax.broadcasted_iota(jnp.int32, (ROWS, CZ), 0)


def lane_matrix():
    gap = np.abs(np.arange(CZ)[:, None] - np.arange(CZ)[None, :])
    return np.tile(gap <= 1, (3, 1)).astype(jnp.bfloat16)


def z_sums(planes, band):
    n = planes.shape[0]
    left = planes.reshape(n * ROWS, CZ)
    terms = []
    for _ in range(band.shape[0] // CZ):
        if terms:
            left = left - terms[-1].astype(F32)
        terms.append(left.astype(jnp.bfloat16))
    sums = jnp.dot(jnp.concatenate(terms, axis=1), band[...], preferred_element_type=F32)
    return sums.reshape(n, ROWS, CZ)


def x_sums(n, plane, emit):
    planes = [plane(0)]
    pair = None
    for x in range(n):
        if x + 1 < n:
            planes.append(plane(x + 1))
        if x % 2 == 0:
            pair = planes[x] + planes[x + 1] if x + 1 < n else planes[x]
            total = pair + planes[x - 1] if x > 0 else pair
        else:
            total = pair + planes[x + 1] if x + 1 < n else pair
        emit(x, total)


def stencil(n, e, band, emit):
    sums = z_sums(e[...], band)

    def plane(x):
        zs = sums[x]
        return zs + pltpu.roll(zs, 1, 0) + pltpu.roll(zs, ROWS - 1, 0)

    x_sums(n, plane, emit)


def coarse_stencil(n, level, e, emit):
    sy, sz = 2 ** (level - 1), 2**level
    lane = lax.broadcasted_iota(jnp.int32, (CROWS, CZ), 1)

    def plane(x):
        p = e[x]
        zs = p + jnp.where(lane >= sz, pltpu.roll(p, sz, 1), 0.0)
        zs = zs + jnp.where(lane < CZ - sz, pltpu.roll(p, CZ - sz, 1), 0.0)
        return zs + pltpu.roll(zs, sy, 0) + pltpu.roll(zs, CROWS - sy, 0)

    x_sums(n, plane, emit)


def z_pairs(a, level):
    sh = 2**level
    bit = (lax.broadcasted_iota(jnp.int32, a.shape, 1) >> level) & 1
    return a + jnp.where(bit == 0, pltpu.roll(a, CZ - sh, 1), pltpu.roll(a, sh, 1))


def blocks1(tmp, x):
    a = tmp[x, pl.ds(1, CROWS, stride=2), :] + tmp[x, pl.ds(2, CROWS, stride=2), :]
    return z_pairs(a, 0)


def blocks2(a):
    bit = lax.broadcasted_iota(jnp.int32, (CROWS, CZ), 0) & 1
    a = a + jnp.where(bit == 0, pltpu.roll(a, CROWS - 1, 0), pltpu.roll(a, 1, 0))
    return z_pairs(a, 1)


def relaxed(e, g, w):
    def emit(x, total):
        e[x] = w[1, x] * e[x] + w[0, x] * (g[x] + total)

    return emit


def pairwise(e, g, dp1, use):
    held = []

    def emit(x, total):
        left = (g[x] + total) - dp1[x] * e[x]
        if x % 2 == 0:
            held.append(left)
        else:
            use(x // 2, held.pop() + left)

    return emit


def vcycle(e0, g0, dp1_0, w0, dp1_1, w1, w2, e1, g1, e2, g2, tmp, band):
    n0, n1, n2 = BX, BX // 2, BX // 4
    for x in range(n0):
        e0[x] = w0[0, x] * g0[x]
    stencil(n0, e0, band, relaxed(e0, g0, w0))

    def to_level1(k, left):
        tmp[k, 0:ROWS, :] = left
        g1[k] = 0.5 * blocks1(tmp, k)

    stencil(n0, e0, band, pairwise(e0, g0, dp1_0, to_level1))
    for x in range(n1):
        e1[x] = w1[0, x] * g1[x]
    coarse_stencil(n1, 1, e1, relaxed(e1, g1, w1))

    def to_level2(k, left):
        g2[k] = 0.5 * blocks2(left)

    coarse_stencil(n1, 1, e1, pairwise(e1, g1, dp1_1, to_level2))
    for x in range(n2):
        e2[x] = w2[0, x] * g2[x]
    for _ in range(3):
        coarse_stencil(n2, 2, e2, relaxed(e2, g2, w2))
    for x in range(n1):
        e1[x] = e1[x] + e2[x // 2]
    for _ in range(2):
        coarse_stencil(n1, 1, e1, relaxed(e1, g1, w1))
    for x in range(n1):
        tmp[x, pl.ds(1, CROWS, stride=2), :] = e1[x]
        tmp[x, pl.ds(2, CROWS, stride=2), :] = e1[x]
        tmp[x, 0:1, :] = jnp.zeros((1, CZ), F32)
    for x in range(n0):
        e0[x] = e0[x] + tmp[x // 2, 0:ROWS, :]
    for _ in range(2):
        stencil(n0, e0, band, relaxed(e0, g0, w0))


def clear_ends(tmp):
    for x in range(BX // 2):
        tmp[x, ROWS:, :] = jnp.zeros((16, CZ), F32)


def send_x(idx, v, out_a, out_b):
    width = out_a.shape[0]
    low, high = 1, BX + 1 - width
    out_a[...] = v[pl.ds(jnp.where(idx[0] == 0, high, low), width)]
    out_b[...] = v[pl.ds(jnp.where(idx[0] == 0, low, high), width)]


def partner_b(idx, in_b):
    return jnp.where((idx[2] + idx[3]) == 0, in_b[idx[0]], 0.0)


def pack_x_kernel(idx, r, s, out_a, out_b, sems):
    a = jnp.where(idx[0] == 0, CX - 2, 0)
    b = jnp.where(idx[0] == 0, 0, CX - 2)
    copies = [
        pltpu.make_async_copy(src.at[pl.ds(first, 2)], out.at[k], sems.at[2 * k + n])
        for k, src in enumerate((r, s))
        for n, (first, out) in enumerate(((a, out_a), (b, out_b)))
    ]
    for copy in copies:
        copy.start()
    for copy in copies:
        copy.wait()


def box_kernel(idx, r, s, in_a, in_b, rbox, sbox, out_a, out_b, pack):
    even = idx[0] == 0
    a = jnp.where(even, CX + 2, 0)
    b = jnp.where(even, 0, CX + 2)
    from_b = partner_b(idx, in_b)
    for k, (src, dst) in enumerate(((r, rbox), (s, sbox))):
        dst[...] = jnp.zeros_like(dst)
        for x in range(CX):
            dst[x + 2, 3 : 3 + CY, :] = src[x]
        for x in range(2):
            dst[a + x, 3 : 3 + CY, :] = in_a[k, x]
            dst[b + x, 3 : 3 + CY, :] = from_b[k, x]
        for x in range(BX):
            pack[0, 4 * x + 2 * k : 4 * x + 2 * k + 2, :] = dst[x, 3:5, :]
            pack[1, 4 * x + 2 * k : 4 * x + 2 * k + 2, :] = dst[x, 33:35, :]
    up = jnp.where(idx[1] == 0, 1, 0)
    out_a[...] = pack[up]
    out_b[...] = pack[1 - up]


def first_kernel(
    idx, rin, sin, in_a, in_b, band,
    r0, v, out_a, out_b, dp1_0, w0, dp1_1, w1, w2,
    got, s0, s1, e1, g1, e2, g2, tmp,
):
    up = jnp.where(idx[1] == 0, 1, 0)
    got[up] = in_a[...]
    got[1 - up] = jnp.where((idx[4] + idx[5]) == 0, in_b[idx[1]], 0.0)
    for k, (src, dst) in enumerate(((rin, r0), (sin, s0))):
        dst[...] = src[...]
        for x in range(BX):
            dst[x, 1:3, :] = got[0, 4 * x + 2 * k : 4 * x + 2 * k + 2, :]
            dst[x, 35:37, :] = got[1, 4 * x + 2 * k : 4 * x + 2 * k + 2, :]

    def coefficients(x, scale, s, inside, dp1, w):
        d = CENTER + scale * s
        if dp1 is not None:
            dp1[x] = d + 1.0
        ratio = RELAX / d
        w[0, x] = jnp.where(inside, ratio, 0.0)
        w[1, x] = jnp.where(inside, (1.0 - RELAX) - ratio, 0.0)

    clear_ends(tmp)
    row = rows()
    for x in range(BX):
        coefficients(x, 1.0, s0[x], (row >= 1) & (row < 37), dp1_0, w0)
    inside = lax.broadcasted_iota(jnp.int32, (CROWS, CZ), 0) < (CY + 4) // 2
    for x in range(BX // 2):
        tmp[x, 0:ROWS, :] = s0[2 * x] + s0[2 * x + 1]
        s1[x] = 0.125 * blocks1(tmp, x)
        coefficients(x, 4.0, s1[x], inside, dp1_1, w1)
    for x in range(BX // 4):
        coefficients(x, 16.0, 0.125 * blocks2(s1[2 * x] + s1[2 * x + 1]), inside, None, w2)
    v[0] = jnp.zeros((ROWS, CZ), F32)
    v[WX - 1] = jnp.zeros((ROWS, CZ), F32)
    vcycle(v.at[pl.ds(1, BX)], r0, dp1_0, w0, dp1_1, w1, w2, e1, g1, e2, g2, tmp, band.at[pl.ds(0, 2 * CZ)])
    send_x(idx, v, out_a, out_b)


def pack_y_kernel(idx, v, in_a, in_b, out_a, out_b, w, pack):
    width = in_a.shape[0]
    x0 = 5 - width
    for x in range(WX):
        w[x, 0:8, :] = v[x, 0:8, :]
        w[x, 8:16, :] = v[x, 32:40, :]
    a = jnp.where(idx[0] == 0, CX + 1, x0)
    b = jnp.where(idx[0] == 0, x0, CX + 1)
    from_b = partner_b(idx, in_b)
    for first, src in ((a, in_a), (b, from_b)):
        for x in range(width):
            w[first + x, 0:8, :] = w[first + x, 0:8, :] + src[x, 0:8, :]
            w[first + x, 8:16, :] = w[first + x, 8:16, :] + src[x, 32:40, :]
    pack[:, pack.shape[1] - 8 :, :] = jnp.zeros((2, 8, CZ), F32)
    for x in range(x0, WX - x0):
        at = width * (x - x0)
        pack[0, at : at + width, :] = w[x, 1 : 1 + width, :]
        pack[1, at : at + width, :] = w[x, 13 - width : 13, :]
    up = jnp.where(idx[1] == 0, 1, 0)
    out_a[...] = pack[up]
    out_b[...] = pack[1 - up]


def assemble(idx, w, v, xa, xb, ya, yb, got):
    width = xa.shape[0]
    size = ya.shape[0]
    x0 = 5 - width
    even = idx[0] == 0
    from_a = idx[1] == 1
    far = jnp.where((idx[4] + idx[5]) == 0, yb[idx[1]], 0.0)
    near = ya[...]
    got[0, 8 : 8 + size, :] = jnp.where(from_a, near, far)
    got[1, 8 : 8 + size, :] = jnp.where(from_a, far, near)
    inner = (idx[2] + idx[3]) == 0
    row = lax.broadcasted_iota(jnp.int32, (8, CZ), 0)
    low_mask = jnp.where((row >= 3) | (idx[4] == 0), 1.0, 0.0)
    high_mask = jnp.where((row < 3) | (idx[5] == 0), 1.0, 0.0)
    for x in range(WX):
        plane = v[x]
        if x0 <= x < 5 or CX + 1 <= x < WX - x0:
            k = x - x0 if x < 5 else x - (CX + 1)
            upper = jnp.where(inner, xb[idx[0], k], 0.0)
            plane = plane + jnp.where(even == (x > 5), xa[k], upper)
        low, middle, high = plane[0:8], plane[8:32], plane[32:40]
        if x0 <= x < WX - x0:
            at = 8 + width * (x - x0)
            take = (row >= x0) & (row < 5)
            low = low + jnp.where(take, got[0, at - x0 : at - x0 + 8, :], 0.0)
            take = (row >= 1) & (row < 1 + width)
            high = high + jnp.where(take, got[1, at - 1 : at + 7, :], 0.0)
        low, high = low * low_mask, high * high_mask
        plane = jnp.concatenate([low, middle, high], axis=0)
        if x < 3:
            plane = plane * jnp.where(idx[2] == 0, 1.0, 0.0)
        if x >= CX + 3:
            plane = plane * jnp.where(idx[3] == 0, 1.0, 0.0)
        w[x] = plane


def box_mask(idx, x):
    row = rows()
    low = jnp.where(idx[4] == 0, 1, 3)
    high = jnp.where(idx[5] == 0, 37, 35)
    m = jnp.where((row >= low) & (row < high), 1.0, 0.0)
    if x < 2:
        m = m * jnp.where(idx[2] == 0, 1.0, 0.0)
    if x >= CX + 2:
        m = m * jnp.where(idx[3] == 0, 1.0, 0.0)
    return m


def next_kernel(
    idx, vin, xa, xb, ya, yb, rin, dp1_0, w0, dp1_1, w1, w2, band,
    z, r, v, out_a, out_b,
    w, got, e1, g1, e2, g2, tmp,
):
    assemble(idx, w, vin, xa, xb, ya, yb, got)
    clear_ends(tmp)
    z[...] = w[pl.ds(3, CX)]

    def emit(x, total):
        if 1 <= x <= BX:
            image = dp1_0[x - 1] * w[x] - total
            r[x - 1] = rin[x - 1] - (STEP * box_mask(idx, x - 1)) * image

    stencil(WX, w, band, emit)
    v[0] = jnp.zeros((ROWS, CZ), F32)
    v[WX - 1] = jnp.zeros((ROWS, CZ), F32)
    vcycle(v.at[pl.ds(1, BX)], r, dp1_0, w0, dp1_1, w1, w2, e1, g1, e2, g2, tmp, band.at[pl.ds(0, 2 * CZ)])
    send_x(idx, v, out_a, out_b)


def lane_sums(values):
    lane = lax.broadcasted_iota(jnp.int32, (1, CZ), 1)
    out = jnp.zeros((1, CZ), F32)
    for k, s in enumerate(values):
        part = jnp.sum(jnp.sum(s, axis=0, keepdims=True), axis=1, keepdims=True)
        out = out + jnp.where(lane == k, part, 0.0)
    return out


def own_rows():
    row = rows()
    return jnp.where((row >= 3) & (row < 3 + CY), 1.0, 0.0)


def dots_kernel(idx, vin, xa, xb, ya, yb, dp1_0, z0, z1, r0, r1, r2, band, z2, u2, sums, w, got):
    assemble(idx, w, vin, xa, xb, ya, yb, got)
    own = own_rows()
    acc = [jnp.zeros((ROWS, CZ), F32) for _ in range(7)]

    def emit(x, total):
        if 3 <= x < 3 + CX:
            a2 = w[x]
            image = dp1_0[x - 1] * a2 - total
            z2[x - 3] = a2
            u2[x - 3] = image
            a0, a1, a2 = z0[x - 3] * own, z1[x - 3] * own, a2 * own
            b0, b1, b2 = r0[x - 1], r1[x - 1], r2[x - 1]
            terms = (a0 * b0, a0 * b1, a0 * b2, a1 * b1, a1 * b2, a2 * b2, a2 * image)
            acc[:] = [s + t for s, t in zip(acc, terms)]

    stencil(WX, w, band, emit)
    sums[...] = jnp.broadcast_to(lane_sums(acc), sums.shape)


def final_kernel(gathered, z0, z1, z2, r0, r1, r2, u2, x_out, r_out, x_part, r_part, sems):
    row = jnp.sum(gathered[...], axis=0, keepdims=True)
    lane = lax.broadcasted_iota(jnp.int32, (1, CZ), 1)
    m00, m01, m02, m11, m12, m22, h22 = (
        jnp.sum(jnp.where(lane == k, row, 0.0), axis=1, keepdims=True) for k in range(7)
    )
    inv = 1.0 / STEP
    h00, h01, h02 = inv * (m00 - m01), inv * (m01 - m02), inv * (m02 - m12)
    h11, h12 = inv * (m11 - m12), inv * (m12 - m22)
    l10, l20 = h01 / h00, h02 / h00
    d1 = h11 - l10 * h01
    q = h12 - l10 * h02
    l21 = q / d1
    d2 = h22 - l20 * h02 - l21 * q
    y1 = m01 - l10 * m00
    y2 = m02 - l20 * m00 - l21 * y1
    c2 = y2 / d2
    c1 = y1 / d1 - l21 * c2
    c0 = m00 / h00 - l10 * c1 - l20 * c2
    f0, f1 = inv * c0, inv * c1
    copies = []
    for x in range(CX):
        xs = c0 * z0[x] + c1 * z1[x] + c2 * z2[x]
        b0, b1 = r0[x + 2], r1[x + 2]
        rs = b0 - f0 * (b0 - b1) - f1 * (b1 - r2[x + 2]) - c2 * u2[x]
        x_part[x] = xs[3 : 3 + CY, :]
        r_part[x] = rs[3 : 3 + CY, :]
        if x % CHUNK == CHUNK - 1:
            part = pl.ds(x + 1 - CHUNK, CHUNK)
            for src, dst in ((x_part, x_out), (r_part, r_out)):
                copies.append(
                    pltpu.make_async_copy(src.at[part], dst.at[part], sems.at[len(copies)])
                )
                copies[-1].start()
    for copy in copies:
        copy.wait()


CHUNK = 8


def call(body, n_in, outs, scratch=(), smem=True, space=pltpu.VMEM, out=pltpu.VMEM):
    in_specs = [pl.BlockSpec(memory_space=space) for _ in range(n_in)]
    kernel = body
    if smem:

        def kernel(*refs):
            body(place(), *refs)

    return pl.pallas_call(
        kernel,
        out_shape=outs,
        in_specs=in_specs,
        out_specs=[pl.BlockSpec(memory_space=out) for _ in outs],
        scratch_shapes=[pltpu.VMEM(s, F32) if isinstance(s, tuple) else s for s in scratch],
        interpret=INTERPRET,
        compiler_params=pltpu.CompilerParams(vmem_limit_bytes=VMEM_LIMIT),
    )


INTERPRET = False
VMEM_LIMIT = 16 * 2**20


def pairs(n_gx, n_gy, axis, odd):
    count = n_gx if axis == 0 else n_gy
    result = []
    for i in range(n_gx):
        for j in range(n_gy):
            here = i if axis == 0 else j
            there = ((here + odd) ^ 1) - odd
            if 0 <= there < count:
                target = (there, j) if axis == 0 else (i, there)
                result.append((i * n_gy + j, target[0] * n_gy + target[1]))
    return result


def solution(mesh):
    n_gx, n_gy = mesh.shape["gx"], mesh.shape["gy"]

    far = [[i * n_gy + j, i * n_gy + j + 1] for i in range(n_gx) for j in range(1, n_gy - 1, 2)]
    far += [[i * n_gy + j, (i + 1) * n_gy + j] for i in range(0, n_gx, 2) for j in (0, n_gy - 1)]
    neighbours = [[i * n_gy + j, (i + 1) * n_gy + j] for i in range(1, n_gx - 1, 2) for j in range(n_gy)]
    neighbours += [[i * n_gy + j, i * n_gy + j + 2] for i in (0, n_gx - 1) for j in range(n_gy) if j % 4 < 2]

    def swap_x(a, b):
        return (
            lax.ppermute(a, AX, pairs(n_gx, n_gy, 0, 0)),
            lax.all_gather(b, AX, axis_index_groups=neighbours),
        )

    def swap_y(a, b):
        a = lax.ppermute(a, AX, pairs(n_gx, n_gy, 1, 0))
        b = lax.all_gather(b, AX, axis_index_groups=far)
        return a, b

    box = sds(BX, ROWS, CZ)
    half = sds(BX // 2, CROWS, CZ)
    quarter = sds(BX // 4, CROWS, CZ)
    weights = [sds(2, BX, ROWS, CZ), half, sds(2, BX // 2, CROWS, CZ), sds(2, BX // 4, CROWS, CZ)]
    wide = sds(WX, ROWS, CZ)
    own = sds(CX, ROWS, CZ)
    coarse = [half.shape, half.shape, quarter.shape, quarter.shape, (BX // 2, ROWS + 16, CZ)]

    def yrows(width):
        return -(-(CX - 4 + 2 * width) * width // 8) * 8

    def on_device(right_side, shift):
        def exchange(v, xa, xb):
            width = xa.shape[0]
            xa, xb = swap_x(xa, xb)
            size = yrows(width)
            ya, yb = call(pack_y_kernel, 3, [sds(size, CZ)] * 2, [(WX, 16, CZ), (2, size, CZ)])(v, xa, xb)
            return (v, xa, xb) + swap_y(ya, yb)

        matrix = jnp.asarray(lane_matrix())
        first = sds(2, 2, CY, CZ)
        xa, xb = call(
            pack_x_kernel, 2, [first, first], [pltpu.SemaphoreType.DMA((4,))], space=pltpu.HBM
        )(*(pltpu.with_memory_space_constraint(a, pltpu.HBM) for a in (right_side, shift)))
        xa, xb = swap_x(xa, xb)
        strip = sds(IROWS, CZ)
        rbox, sbox, ya, yb = call(box_kernel, 4, [box, box, strip, strip], [(2, IROWS, CZ)])(right_side, shift, xa, xb)
        ya, yb = swap_y(ya, yb)
        r0, v, xa, xb, *coefs = call(
            first_kernel,
            5,
            [box, wide, sds(5, ROWS, CZ), sds(5, ROWS, CZ), box] + weights,
            [(2, IROWS, CZ), box.shape, half.shape] + coarse,
        )(rbox, sbox, ya, yb, matrix)
        residuals, images = [r0], []
        for width in (5, 3):
            z, r, v, xa, xb = call(
                next_kernel,
                12,
                [own, box, wide, sds(width, ROWS, CZ), sds(width, ROWS, CZ)],
                [wide.shape, (2, yrows(5) + 16, CZ)] + coarse,
            )(*exchange(v, xa, xb), residuals[-1], *coefs, matrix)
            images.append(z)
            residuals.append(r)
        z2, u2, sums = call(
            dots_kernel, 12, [own, own, sds(n_gx * n_gy, CZ)], [wide.shape, (2, yrows(3) + 16, CZ)]
        )(*exchange(v, xa, xb), coefs[0], *images, *residuals, matrix)
        gathered = lax.all_to_all(sums, AX, 0, 0, tiled=True)
        x, r = call(
            final_kernel,
            8,
            [sds(CX, CY, CZ)] * 2,
            [(CX, CY, CZ), (CX, CY, CZ), pltpu.SemaphoreType.DMA((2 * CX // CHUNK,))],
            smem=False,
            out=pltpu.HBM,
        )(gathered, *images, z2, *residuals, u2)
        return x, r

    spec = P("gx", "gy", None)
    return jax.shard_map(
        on_device, mesh=mesh, in_specs=(spec, spec), out_specs=(spec, spec), check_vma=False
    )
```
